32 devices in a mesh: groups: 2 (over x), section: 2 (over core), expert: 8 (over z, y).
Axes of the slice: x: 2, y: 2, z: 4, core: 2. Of those that a mesh axis runs over, the one named last changes fastest.
Arguments:
- tokens: bfloat16 [2, 128, 6144], P(None, ('groups', 'expert')), parts along dimension 1, may hold values from -6 to 6
- expert_ids: int32 [2, 2, 128, 2], P('section', None, ('groups', 'expert')), parts along dimension 2, may hold values from 0 to 7, all different within a row; in each aligned block of 8 rows (0 to 7, 8 to 15, ..., all dimensions but the last counted through in order) at most 4 rows name the same one
- norm_gain: bfloat16 [2, 6144], P('section'), may hold values from 0.25 to 1.75
- router: bfloat16 [2, 6144, 8], P('section'), may hold values from -0.078125 to 0.078125
- w_gate: bfloat16 [2, 6144, 16384], P('section', None, 'expert'), may hold values from -0.078125 to 0.078125
- w_up: bfloat16 [2, 6144, 16384], P('section', None, 'expert'), may hold values from -0.078125 to 0.078125
- w_down: bfloat16 [2, 16384, 6144], P('section', 'expert'), may hold values from -0.0625 to 0.0625
Outputs:
- mixed: bfloat16 [2, 128, 6144], P('section', ('groups', 'expert')), parts along dimension 1
The draws below stay inside these ranges and needn't reach their ends.
There are 2 independent parts, one for each index of `groups`. The reference program is written for one: setup_inputs(seed, part) draws one part's arguments, and reference() takes and returns one part's arrays. A program takes and returns all parts, laid end to end along the dimension named above; an argument that names none is the same for every part. Nothing has to cross between parts.
Inputs may be any that keep to these rules, and one draw needn't show every extreme that they name: `expert_ids`: in each aligned block of 8 rows (one index of expert, one micro-batch, one layer) no expert is named by more than 4 of the pairs; a token's two ids differ.
All inputs are finite; a program needn't handle non-finite values.
Results may differ from the reference program's by a relative error of at most 0.0055.
Values may be sent and summed in bfloat16 or wider, within the bound.
No kernel may reach another device: no remote copies, remote signals or barrier semaphores. Data moves between devices by JAX's collectives and lax.ppermute only.
A program may use at most 128 MiB of HBM per device.

```python
import math
import jax
import jax.numpy as jnp
import numpy as np
from jax import lax

D = 6144
FF_WIN = 8192
NEXP = 8
TOPK = 2
E_WIN = 2
TOK_DEV = 8
CAP = 4
SPLIT = 4
FF_DEV = 2048
MICRO = 2
LAYERS = 2
TOKENS = 64
N_EXPERT = 8


def block_scale(own_key, extent, cuts, low, largest):
    def one(axis_at, parts):
        steps = jax.random.uniform(jax.random.fold_in(jax.random.fold_in(own_key, 6), axis_at), (parts,), jnp.float32, low / len(cuts), largest / len(cuts))
        return jnp.repeat(jnp.exp(steps), extent[axis_at] // parts).reshape((-1,) + (1,) * (len(extent) - axis_at - 1))

    level = one(*cuts[0])
    for cut in cuts[1:]:
        level = level * one(*cut)
    return level


def shared_out(rng, own, number, rows, amount, top, bound, skew):
    ranking = jax.random.permutation(rng, amount)
    crowded, common = shares(amount, rows * top, bound, skew, True), shares(amount, rows * top, bound, skew, False)
    places = jnp.arange(amount)

    def named(lengths, turn):
        used = int((lengths > 0).sum())
        fixed = max(1, used // 4)
        passed = fixed + (places - fixed + turn * (used - fixed)) % max(1, amount - fixed)
        return jnp.zeros((amount,), jnp.int32).at[ranking[jnp.where(places < fixed, places, passed)]].set(jnp.asarray(lengths, jnp.int32))

    lengths = jnp.where(number % 4 == 0, named(crowded, number // 4), named(common, number - number // 4 - 1))
    mixed = jax.random.permutation(jax.random.fold_in(own, 3), amount)
    source_of, sink = mixed[0:amount // 2 * 2:2], mixed[1:amount // 2 * 2:2]
    margin = jnp.minimum(lengths[source_of] - 1, bound - lengths[sink]) // 2
    margin = jnp.where((source_of == ranking[0]) | (sink == ranking[0]) | (lengths[sink] == 0), 0, jnp.maximum(margin, 0))
    passed = jax.random.randint(jax.random.fold_in(own, 4), (amount // 2,), 0, 1 << 20) % (margin + 1)
    lengths = lengths.at[source_of].add(-passed).at[sink].add(passed)
    labels = jnp.searchsorted(jnp.cumsum(lengths), jnp.arange(rows * top), side="right").astype(jnp.int32)
    listing = labels.reshape(top, rows).T
    listing = listing[jax.random.permutation(jax.random.fold_in(own, 1), rows)]
    turn = jax.random.randint(jax.random.fold_in(own, 2), (rows, 1), 0, top)
    return jnp.take_along_axis(listing, (jnp.arange(top)[None, :] + turn) % top, axis=1)


def shares(amount, total, reach, skew, full):
    loads = [(1 << 20) // math.isqrt(rank ** skew) + 1 for rank in range(1, amount + 1)]
    largest = reach if full else min(reach, max(-(-total // amount), total * loads[0] // sum(loads)))
    least = 1 if total - largest >= amount - 1 else 0
    counts, rest = [largest] + [least] * (amount - 1), total - largest - least * (amount - 1)
    while rest > 0:
        candidates = [i for i in range(1, amount) if counts[i] < largest] or [i for i in range(1, amount) if counts[i] < reach]
        pool, left = sum([loads[i] for i in candidates]), rest
        for i in candidates:
            extra = min(reach - counts[i], max(1, left * loads[i] // pool), rest)
            counts[i] = counts[i] + extra
            rest = rest - extra
    return np.array(counts)


def normal_values(stream_key, shape, spread, reach, shards=(), kind=jnp.bfloat16):
    level = block_scale(stream_key, shape, shards, -0.22, 0.18) if shards else 1.0
    result = jax.random.normal(stream_key, shape, jnp.float32) * spread * level
    return jnp.minimum(jnp.maximum(result, -reach), reach).astype(kind)


def setup_inputs(seed: int = 0, part: int = 0) -> dict:
    keys = jax.random.split(jax.random.key(seed), 8)
    part_keys = jax.random.split(jax.random.fold_in(keys[7], part), 8)
    tokens = normal_values(part_keys[0], (MICRO, TOKENS, D), 1.0, 6.0, ((1, 8),))
    expert_ids_keys = jax.random.split(jax.random.fold_in(part_keys[1], 1), LAYERS * MICRO * TOKENS // TOK_DEV)
    expert_ids_turns = jax.random.permutation(jax.random.fold_in(part_keys[1], 3), LAYERS * MICRO * TOKENS // TOK_DEV)
    expert_ids = jax.vmap(lambda own, number: shared_out(jax.random.fold_in(part_keys[1], 2), own, number, TOK_DEV, NEXP, TOPK, CAP, 2))(expert_ids_keys, expert_ids_turns).reshape((LAYERS, MICRO, TOKENS, TOPK))
    norm_gain = jnp.clip(1.0 + 0.15 * jax.random.normal(keys[2], (LAYERS, D), jnp.float32), 0.25, 1.75).astype(jnp.bfloat16)
    router = normal_values(keys[3], (LAYERS, D, NEXP), D ** -0.5, 0.078125, ((0, 2),))
    w_gate = normal_values(keys[4], (LAYERS, D, E_WIN * FF_WIN), D ** -0.5, 0.078125, ((0, 2), (2, 8)))
    w_up = normal_values(keys[5], (LAYERS, D, E_WIN * FF_WIN), D ** -0.5, 0.078125, ((0, 2), (2, 8)))
    w_down = normal_values(keys[6], (LAYERS, E_WIN * FF_WIN, D), FF_WIN ** -0.5, 0.0625, ((0, 2), (1, 8)))
    return {"tokens": tokens, "expert_ids": expert_ids, "norm_gain": norm_gain, "router": router, "w_gate": w_gate, "w_up": w_up, "w_down": w_down}


epsilon = 1e-05

def normalize(stream, gain):
    values = stream.astype(jnp.float32)
    scale = lax.rsqrt(lax.optimization_barrier(jnp.mean(values * values, axis=-1, keepdims=True)) + epsilon)
    return (values * scale * gain.astype(jnp.float32)).astype(jnp.bfloat16)

def route(normed, chosen_ids, router_matrix):
    logits = jnp.dot(normed, router_matrix, preferred_element_type=jnp.float32)
    chosen_hot = (chosen_ids[..., None] == jnp.arange(NEXP, dtype=jnp.int32)).astype(jnp.float32)
    chosen = lax.optimization_barrier(jnp.sum(chosen_hot * logits[:, None, :], axis=-1))
    first = jax.nn.sigmoid(chosen[:, 0] - chosen[:, 1])
    second = jax.nn.sigmoid(chosen[:, 1] - chosen[:, 0])
    gates = jnp.stack([first, second], axis=1)
    flat = chosen_hot.reshape(-1, NEXP)
    before = jnp.cumsum(flat, axis=0) - flat
    position = lax.optimization_barrier(jnp.sum(before * flat, axis=-1))
    slot_hot = (position[:, None] == jnp.arange(CAP, dtype=jnp.float32)).astype(jnp.float32)
    assign = (flat[:, :E_WIN, None] * slot_hot[:, None, :]).reshape(-1, TOPK, E_WIN * CAP)
    pick = lax.optimization_barrier(jnp.sum(assign, axis=1))
    weights = lax.optimization_barrier(jnp.sum(gates[:, :, None] * assign, axis=1))
    return (pick, weights)

def layer(stream, chosen_ids, gain, router_matrix, gate_matrix, up_matrix, down_matrix):
    normed = normalize(stream, gain)
    blocks = normed.reshape(N_EXPERT, TOK_DEV, D)
    id_blocks = chosen_ids.reshape(N_EXPERT, TOK_DEV, TOPK)
    pick, weights = jax.vmap(lambda rows_in, ids_in: route(rows_in, ids_in, router_matrix))(blocks, id_blocks)
    packed = jnp.einsum('ntc,ntd->ncd', pick, blocks.astype(jnp.float32)).astype(jnp.bfloat16)

    def one_slice(total, device_index):
        expert_index = device_index // SPLIT
        rows = lax.dynamic_slice_in_dim(packed, (expert_index * CAP).astype(jnp.int32), CAP, 1).reshape(N_EXPERT * CAP, D)
        start = (device_index * FF_DEV).astype(jnp.int32)
        gate_part = lax.dynamic_slice_in_dim(gate_matrix, start, FF_DEV, 1)
        up_part = lax.dynamic_slice_in_dim(up_matrix, start, FF_DEV, 1)
        down_part = lax.dynamic_slice_in_dim(down_matrix, start, FF_DEV, 0)
        gate_value = jnp.dot(rows, gate_part, preferred_element_type=jnp.float32)
        up_value = jnp.dot(rows, up_part, preferred_element_type=jnp.float32)
        hidden = (jax.nn.silu(gate_value) * up_value).astype(jnp.bfloat16)
        term = jnp.dot(hidden, down_part, preferred_element_type=jnp.float32).astype(jnp.bfloat16)
        term = term.astype(jnp.float32).reshape(N_EXPERT, CAP, D)
        select = (jnp.arange(E_WIN, dtype=jnp.int32) == expert_index).astype(jnp.float32)
        return (total + select[None, :, None, None] * term[:, None, :, :], None)
    start_total = jnp.zeros((N_EXPERT, E_WIN, CAP, D), jnp.float32)
    total, unused = lax.scan(one_slice, start_total, jnp.arange(N_EXPERT, dtype=jnp.int32))
    expert_out = total.reshape(N_EXPERT, E_WIN * CAP, D)
    moe = jnp.einsum('ntc,ncd->ntd', weights, expert_out, precision=lax.Precision.HIGHEST)
    return (stream.astype(jnp.float32) + moe.reshape(TOKENS, D)).astype(jnp.bfloat16)

def reference(tokens, expert_ids, norm_gain, router, w_gate, w_up, w_down):
    results = []
    for micro_index in range(MICRO):
        stream = tokens[micro_index]
        for layer_index in range(LAYERS):
            stream = layer(stream, expert_ids[layer_index, micro_index], norm_gain[layer_index], router[layer_index], w_gate[layer_index], w_up[layer_index], w_down[layer_index])
        results.append(stream)
    return jnp.stack(results)
```

```python
import jax
import jax.numpy as jnp
from jax import lax
from jax.experimental import pallas as pl
from jax.experimental.pallas import tpu as pltpu
from jax.sharding import PartitionSpec as P

NEXP = 8
E_WIN = 2
CAP = 4
MIB = 1 << 20
DIRECT = 8


epsilon = 1e-05

VMEM = pl.BlockSpec(memory_space=pltpu.VMEM)
ANY = pl.BlockSpec(memory_space=pl.ANY)
f32 = jnp.float32
bf16 = jnp.bfloat16


def swap(value):
    count = lax.axis_size("section")
    return lax.ppermute(value, "section", [(s, (s + 1) % count) for s in range(count)])


def prepare(values, layer, ids_own, ids_other, gain_own, gain_other, router_own, router_other, near_ref, far_ref, weights_ref):
    section = lax.axis_index("section")
    split = lax.axis_size("expert") // E_WIN
    near = lax.axis_index("expert") // split
    mine = section == layer
    gain = jnp.where(mine, gain_own[...].astype(f32), gain_other[...].astype(f32))
    router = jnp.where(mine, router_own[...].astype(f32), router_other[...].astype(f32)).astype(bf16)
    ids = jnp.where(mine, ids_own[section], ids_other[section])
    scale = lax.rsqrt(jnp.mean(values * values, axis=-1, keepdims=True) + epsilon)
    normed = (values * scale * gain).astype(bf16)
    logits = lax.dot_general(normed, router, (((1,), (1,)), ((), ())), preferred_element_type=f32)
    tokens = values.shape[0]
    expert = lax.broadcasted_iota(jnp.int32, (tokens, NEXP), 1)
    first = (ids[:, 0:1] == expert).astype(f32)
    second = (ids[:, 1:2] == expert).astype(f32)
    chosen_first = jnp.sum(first * logits, axis=-1, keepdims=True)
    chosen_second = jnp.sum(second * logits, axis=-1, keepdims=True)
    gate_first = jax.nn.sigmoid(chosen_first - chosen_second)
    gate_second = jax.nn.sigmoid(chosen_second - chosen_first)
    named = first + second
    gates = first * gate_first + second * gate_second
    row = lax.broadcasted_iota(jnp.int32, (tokens, tokens), 0)
    column = lax.broadcasted_iota(jnp.int32, (tokens, tokens), 1)
    earlier = jnp.dot((column < row).astype(f32), named, preferred_element_type=f32)
    lane = lax.broadcasted_iota(jnp.int32, (tokens, E_WIN * CAP), 1)
    is_near = lane < CAP
    slot = jnp.where(is_near, lane, lane - CAP).astype(f32)

    def spread(table):
        low, high = table[:, 0:1], table[:, 1:2]
        return jnp.where(is_near == (near == 0), low, high)

    pick = spread(named) * (spread(earlier) == slot).astype(f32)
    weights_ref[...] = spread(gates) * pick
    packed = lax.dot_general(
        pick.astype(bf16), normed, (((0,), (0,)), ((), ())), preferred_element_type=f32
    )
    near_ref[0] = packed[:CAP].astype(bf16)
    far_ref[0] = packed[CAP:].astype(bf16)


def combine(values, weights_ref, returned):
    blocks = []
    for ref in returned:
        for index in range(ref.shape[0]):
            blocks.append(ref[index].astype(f32))
    split = len(blocks) // E_WIN
    result = values
    for side in range(E_WIN):
        total = blocks[side * split]
        for block in blocks[side * split + 1:(side + 1) * split]:
            total = total + block
        for slot in range(CAP):
            column = side * CAP + slot
            result = result + weights_ref[:, column:column + 1] * total[slot:slot + 1, :]
    return result.astype(bf16)


def first_kernel(tokens, *refs):
    prepare(tokens[lax.axis_index("section")].astype(f32), 0, *refs)


def middle_kernel(count, layer, tokens, *refs):
    returned, refs = refs[:count], refs[count:]
    weights, refs = refs[0], refs[1:]
    params, outs = refs[:6], refs[6:]
    stream = combine(tokens[lax.axis_index("section")].astype(f32), weights, returned)
    outs[0][...] = stream
    prepare(stream.astype(f32), layer, *params, *outs[1:])


def final_kernel(count, stream, *refs):
    returned, weights, out = refs[:count], refs[count], refs[count + 1]
    out[0] = combine(stream[...].astype(f32), weights, returned)


def select_kernel(layer, own, crossed, *outs):
    mine = lax.axis_index("section") == layer
    row = 0
    pieces = [(out, index) for out in outs for index in range(out.shape[0])]
    for low in range(0, len(pieces), 2):
        lines = pl.ds(low * CAP, 2 * CAP)
        value = jnp.where(mine, own[lines, :].astype(f32), crossed[lines, :].astype(f32))
        for at, (out, index) in enumerate(pieces[low:low + 2]):
            out[index] = value[at * CAP:(at + 1) * CAP].astype(bf16)


def expert_kernel(layer, count, *refs):
    inputs, refs = refs[:2 * count], refs[2 * count:]
    gate_ref, down_ref, up_hbm, own_out, other_out = refs[:5]
    rows_ref, up_buf, hidden_ref, total, up_sems = refs[5:]
    half, width = own_out.shape
    units = gate_ref.shape[1]
    pieces, depth, block = up_buf.shape
    blocks = units // block
    strip = width // 8

    def fetch_up(index, piece):
        return pltpu.make_async_copy(
            up_hbm.at[pl.ds(piece * depth, depth), pl.ds(index * block, block)],
            up_buf.at[piece],
            up_sems.at[piece],
        )

    for piece in range(pieces):
        fetch_up(0, piece).start()
    places = [(ref, index) for ref in inputs for index in range(ref.shape[0])]
    for low in range(0, len(places), 2):
        pair = [ref[index].astype(f32) for ref, index in places[low:low + 2]]
        rows_ref[pl.ds(low * CAP, 2 * CAP), :] = jnp.concatenate(pair, axis=0).astype(bf16)

    def enter(index):
        columns = pl.ds(pl.multiple_of(index * block, block), block)
        gate_value = jnp.dot(rows_ref[...], gate_ref[:, columns], preferred_element_type=f32)
        up_value = jnp.zeros((2 * half, block), f32)
        for piece in range(pieces):
            fetch_up(index, piece).wait()
            up_value += jnp.dot(
                rows_ref[:, pl.ds(piece * depth, depth)], up_buf[piece], preferred_element_type=f32
            )

            @pl.when(index + 1 < blocks)
            def _():
                fetch_up(index + 1, piece).start()

        return (jax.nn.silu(gate_value) * up_value).astype(bf16)

    def leave(index, hidden, last):
        lines = pl.ds(pl.multiple_of(index * block, block), block)
        for start in range(0, width, strip):
            columns = pl.ds(start, strip)
            value = total[:, columns] + jnp.dot(
                hidden, down_ref[lines, columns], preferred_element_type=f32
            )
            if last:
                value = value.astype(bf16)
                own_out[:, columns] = value[:half]
                other_out[:, columns] = value[half:]
            else:
                total[:, columns] = value

    total[...] = jnp.zeros_like(total)
    hidden_ref[...] = enter(0)
    if blocks > 1:

        @pl.loop(1, blocks)
        def _(index):
            hidden = hidden_ref[...]
            leave(index - 1, hidden, False)
            hidden_ref[...] = enter(index)

    leave(blocks - 1, hidden_ref[...], True)


def call(kernel, outs, args, specs=None, limit=2 * MIB, scratch=(), flops=10**6):
    many = isinstance(outs, (tuple, list))
    return pl.pallas_call(
        kernel,
        out_shape=tuple(outs) if many else outs,
        in_specs=specs or [VMEM] * len(args),
        out_specs=(VMEM,) * len(outs) if many else VMEM,
        scratch_shapes=list(scratch),
        compiler_params=pltpu.CompilerParams(vmem_limit_bytes=limit),
        cost_estimate=pl.CostEstimate(flops=flops, bytes_accessed=10**5, transcendentals=0),
    )(*args)


def shape(*sizes, dtype=bf16):
    return jax.ShapeDtypeStruct(sizes, dtype)


def experts(layer, own, other, gate_matrix, up_matrix, down_matrix):
    half = CAP * sum(block.shape[0] for block in own)
    width, units = gate_matrix.shape
    block = min(256, units)
    pieces = 8
    depth = width // pieces
    scratch = (
        pltpu.VMEM((2 * half, width), bf16),
        pltpu.VMEM((pieces, depth, block), bf16),
        pltpu.VMEM((2 * half, block), bf16),
        pltpu.VMEM((2 * half, width), f32),
        pltpu.SemaphoreType.DMA((pieces,)),
    )
    count = len(own)
    limit = 2 * width * block + 20 * half * width + 2 * MIB
    args = (
        *own,
        *other,
        STAGE_G(gate_matrix),
        STAGE_D(down_matrix),
        pltpu.with_memory_space_constraint(up_matrix, pltpu.HBM),
    )
    return call(
        lambda *refs: expert_kernel(layer, count, *refs),
        (shape(half, width), shape(half, width)),
        args,
        [VMEM] * (2 * count + 2) + [ANY],
        limit,
        scratch,
        12 * half * width * units,
    )


STAGE_G = STAGE_D = lambda x: pltpu.with_memory_space_constraint(x, pltpu.VMEM)


def exchange(near, far):
    devices = lax.axis_size("expert")
    split = devices // E_WIN
    if devices <= DIRECT:
        blocks = [near]
        for step in range(1, devices):
            pairs = [(i, i ^ step) for i in range(devices)]
            blocks.append(lax.ppermute(near if step < split else far, "expert", pairs))
        return blocks
    low = lax.axis_index("expert") < split
    first, second = jnp.where(low, near, far), jnp.where(low, far, near)
    outgoing = jnp.concatenate([jnp.repeat(first, split, axis=0), jnp.repeat(second, split, axis=0)])
    return [lax.all_to_all(outgoing, "expert", 0, 0, tiled=True)]


def give_back(blocks):
    devices = lax.axis_size("expert")
    if devices <= DIRECT:
        result = [blocks[0]]
        for step in range(1, devices):
            pairs = [(i, i ^ step) for i in range(devices)]
            result.append(lax.ppermute(blocks[step], "expert", pairs))
        return result
    split = devices // E_WIN
    returned = lax.all_to_all(blocks[0], "expert", 0, 0, tiled=True)
    turned = jnp.roll(returned, split, axis=0)
    return [jnp.where(lax.axis_index("expert") < split, returned, turned)]


def body(tokens, expert_ids, norm_gain, router, w_gate, w_up, w_down):
    layers = lax.axis_size("section")
    width = tokens.shape[-1]
    rows = tokens.shape[1]
    ids_own, gain_own, router_own = expert_ids[0], norm_gain, router[0].T
    params = (ids_own, swap(ids_own), gain_own, swap(gain_own), router_own, swap(router_own))
    slots = (shape(1, CAP, width), shape(1, CAP, width), shape(rows, E_WIN * CAP, dtype=f32))
    near, far, weights = call(first_kernel, slots, (tokens, *params))
    stream = tokens
    for layer in range(layers):
        own = exchange(near, far)
        other = [swap(block) for block in own]
        own_terms, other_terms = experts(layer, own, other, w_gate[0], w_up[0], w_down[0])
        crossed = swap(other_terms)
        count = len(own)
        extra = 24 * CAP * sum(block.shape[0] for block in own) * width
        chosen = call(
            lambda *refs, layer=layer: select_kernel(layer, *refs),
            [shape(*block.shape) for block in own],
            (own_terms, crossed),
            limit=2 * MIB + extra // 2,
        )
        returned = give_back(chosen)
        if layer < layers - 1:
            stream, near, far, weights = call(
                lambda *refs, layer=layer: middle_kernel(count, layer + 1, *refs),
                (shape(rows, width), *slots),
                (stream, *returned, weights, *params),
                limit=2 * MIB + extra // 2,
            )
        else:
            return call(
                lambda *refs: final_kernel(count, *refs),
                shape(1, rows, width),
                (stream, *returned, weights),
                limit=2 * MIB + extra // 2,
            )


def solution(mesh):
    in_specs = (
        P(None, ("groups", "expert"), None),
        P("section", None, ("groups", "expert"), None),
        P("section", None),
        P("section", None, None),
        P("section", None, "expert"),
        P("section", None, "expert"),
        P("section", "expert", None),
    )
    out_specs = P("section", ("groups", "expert"), None)
    return jax.shard_map(body, mesh=mesh, in_specs=in_specs, out_specs=out_specs, check_vma=False)
```

```python
import jax
import jax.numpy as jnp
from jax import lax
from jax.experimental import pallas as pl
from jax.experimental.pallas import tpu as pltpu
from jax.sharding import PartitionSpec as P

NEXP = 8
E_WIN = 2
CAP = 4
MIB = 1 << 20
DIRECT = 8


epsilon = 1e-05

VMEM = pl.BlockSpec(memory_space=pltpu.VMEM)
ANY = pl.BlockSpec(memory_space=pl.ANY)
f32 = jnp.float32
bf16 = jnp.bfloat16


def swap(value):
    count = lax.axis_size("section")
    return lax.ppermute(value, "section", [(s, (s + 1) % count) for s in range(count)])


def prepare(values, layer, ids_own, ids_other, gain_own, gain_other, router_own, router_other, near_ref, far_ref, weights_ref):
    section = lax.axis_index("section")
    split = lax.axis_size("expert") // E_WIN
    near = lax.axis_index("expert") // split
    mine = section == layer
    gain = jnp.where(mine, gain_own[...].astype(f32), gain_other[...].astype(f32))
    router = jnp.where(mine, router_own[...].astype(f32), router_other[...].astype(f32)).astype(bf16)
    ids = jnp.where(mine, ids_own[section], ids_other[section])
    scale = lax.rsqrt(jnp.mean(values * values, axis=-1, keepdims=True) + epsilon)
    normed = (values * scale * gain).astype(bf16)
    logits = lax.dot_general(normed, router, (((1,), (1,)), ((), ())), preferred_element_type=f32)
    tokens = values.shape[0]
    expert = lax.broadcasted_iota(jnp.int32, (tokens, NEXP), 1)
    first = (ids[:, 0:1] == expert).astype(f32)
    second = (ids[:, 1:2] == expert).astype(f32)
    chosen_first = jnp.sum(first * logits, axis=-1, keepdims=True)
    chosen_second = jnp.sum(second * logits, axis=-1, keepdims=True)
    gate_first = jax.nn.sigmoid(chosen_first - chosen_second)
    gate_second = jax.nn.sigmoid(chosen_second - chosen_first)
    named = first + second
    gates = first * gate_first + second * gate_second
    row = lax.broadcasted_iota(jnp.int32, (tokens, tokens), 0)
    column = lax.broadcasted_iota(jnp.int32, (tokens, tokens), 1)
    earlier = jnp.dot((column < row).astype(f32), named, preferred_element_type=f32)
    lane = lax.broadcasted_iota(jnp.int32, (tokens, E_WIN * CAP), 1)
    is_near = lane < CAP
    slot = jnp.where(is_near, lane, lane - CAP).astype(f32)

    def spread(table):
        low, high = table[:, 0:1], table[:, 1:2]
        return jnp.where(is_near == (near == 0), low, high)

    pick = spread(named) * (spread(earlier) == slot).astype(f32)
    weights_ref[...] = spread(gates) * pick
    packed = lax.dot_general(
        pick.astype(bf16), normed, (((0,), (0,)), ((), ())), preferred_element_type=f32
    )
    near_ref[0] = packed[:CAP].astype(bf16)
    far_ref[0] = packed[CAP:].astype(bf16)


def combine(values, weights_ref, returned):
    blocks = []
    for ref in returned:
        for index in range(ref.shape[0]):
            blocks.append(ref[index].astype(f32))
    split = len(blocks) // E_WIN
    result = values
    for side in range(E_WIN):
        total = blocks[side * split]
        for block in blocks[side * split + 1:(side + 1) * split]:
            total = total + block
        for slot in range(CAP):
            column = side * CAP + slot
            result = result + weights_ref[:, column:column + 1] * total[slot:slot + 1, :]
    return result.astype(bf16)


def first_kernel(tokens, *refs):
    prepare(tokens[lax.axis_index("section")].astype(f32), 0, *refs)


def middle_kernel(count, layer, tokens, *refs):
    returned, refs = refs[:count], refs[count:]
    weights, refs = refs[0], refs[1:]
    params, outs = refs[:6], refs[6:]
    stream = combine(tokens[lax.axis_index("section")].astype(f32), weights, returned)
    outs[0][...] = stream
    prepare(stream.astype(f32), layer, *params, *outs[1:])


def final_kernel(count, stream, *refs):
    returned, weights, out = refs[:count], refs[count], refs[count + 1]
    out[0] = combine(stream[...].astype(f32), weights, returned)


def select_kernel(layer, own, crossed, *outs):
    mine = lax.axis_index("section") == layer
    row = 0
    pieces = [(out, index) for out in outs for index in range(out.shape[0])]
    for low in range(0, len(pieces), 2):
        lines = pl.ds(low * CAP, 2 * CAP)
        value = jnp.where(mine, own[lines, :].astype(f32), crossed[lines, :].astype(f32))
        for at, (out, index) in enumerate(pieces[low:low + 2]):
            out[index] = value[at * CAP:(at + 1) * CAP].astype(bf16)


def expert_kernel(layer, count, *refs):
    inputs, refs = refs[:2 * count], refs[2 * count:]
    gate_ref, up_hbm, down_hbm, own_out, other_out = refs[:5]
    rows_ref, up_buf, down_buf, gate_sum, up_sum, hidden_ref, total, up_sems, down_sems = refs[5:]
    half, width = own_out.shape
    units = gate_ref.shape[1]
    up_slots, depth, _ = up_buf.shape
    down_slots, block, _ = down_buf.shape
    steps, blocks = width // depth, units // block
    strip = width // 8

    def fetch_up(index, slot):
        lines = pl.ds(pl.multiple_of(index * depth, depth), depth)
        return pltpu.make_async_copy(up_hbm.at[lines], up_buf.at[slot], up_sems.at[slot])

    def fetch_down(index):
        slot = index % down_slots
        return pltpu.make_async_copy(
            down_hbm.at[pl.ds(index * block, block)], down_buf.at[slot], down_sems.at[slot]
        )

    for slot in range(up_slots):
        fetch_up(slot, slot).start()
    places = [(ref, index) for ref in inputs for index in range(ref.shape[0])]
    for low in range(0, len(places), 2):
        pair = [ref[index].astype(f32) for ref, index in places[low:low + 2]]
        rows_ref[pl.ds(low * CAP, 2 * CAP), :] = jnp.concatenate(pair, axis=0).astype(bf16)
    gate_sum[...] = jnp.zeros_like(gate_sum)
    up_sum[...] = jnp.zeros_like(up_sum)

    def enter(index, slot):
        lines = pl.ds(pl.multiple_of(index * depth, depth), depth)
        rows = rows_ref[:, lines]
        gate_sum[...] += jnp.dot(rows, gate_ref[lines, :], preferred_element_type=f32)
        fetch_up(index, slot).wait()
        up_sum[...] += jnp.dot(rows, up_buf[slot], preferred_element_type=f32)

    turns = steps // up_slots

    @pl.loop(0, turns - 1)
    def _(turn):
        for slot in range(up_slots):
            enter(turn * up_slots + slot, slot)
            fetch_up((turn + 1) * up_slots + slot, slot).start()

    for index in range(min(down_slots, blocks)):
        fetch_down(index).start()
    for slot in range(up_slots):
        enter((turns - 1) * up_slots + slot, slot)
    hidden_ref[...] = (jax.nn.silu(gate_sum[...]) * up_sum[...]).astype(bf16)

    for index in range(blocks):
        fetch_down(index).wait()
        hidden = hidden_ref[:, pl.ds(index * block, block)]
        for start in range(0, width, strip):
            columns = pl.ds(start, strip)
            value = jnp.dot(
                hidden, down_buf[index % down_slots, :, columns], preferred_element_type=f32
            )
            if index > 0:
                value += total[:, columns]
            if index == blocks - 1:
                value = value.astype(bf16)
                own_out[:, columns] = value[:half]
                other_out[:, columns] = value[half:]
            else:
                total[:, columns] = value
        if index + down_slots < blocks:
            fetch_down(index + down_slots).start()


def call(kernel, outs, args, specs=None, limit=2 * MIB, scratch=(), flops=10**6):
    many = isinstance(outs, (tuple, list))
    return pl.pallas_call(
        kernel,
        out_shape=tuple(outs) if many else outs,
        in_specs=specs or [VMEM] * len(args),
        out_specs=(VMEM,) * len(outs) if many else VMEM,
        scratch_shapes=list(scratch),
        compiler_params=pltpu.CompilerParams(vmem_limit_bytes=limit),
        cost_estimate=pl.CostEstimate(flops=flops, bytes_accessed=10**5, transcendentals=0),
    )(*args)


def shape(*sizes, dtype=bf16):
    return jax.ShapeDtypeStruct(sizes, dtype)


def experts(layer, own, other, gate_matrix, up_matrix, down_matrix):
    half = CAP * sum(block.shape[0] for block in own)
    width, units = gate_matrix.shape
    block = min(256, units)
    depth = width // 12
    up_slots, down_slots = 4, min(5, units // block)
    scratch = (
        pltpu.VMEM((2 * half, width), bf16),
        pltpu.VMEM((up_slots, depth, units), bf16),
        pltpu.VMEM((down_slots, block, width), bf16),
        pltpu.VMEM((2 * half, units), f32),
        pltpu.VMEM((2 * half, units), f32),
        pltpu.VMEM((2 * half, units), bf16),
        pltpu.VMEM((2 * half, width), f32),
        pltpu.SemaphoreType.DMA((up_slots,)),
        pltpu.SemaphoreType.DMA((down_slots,)),
    )
    count = len(own)
    limit = 2 * up_slots * depth * units + 2 * down_slots * block * width
    limit += 20 * half * width + 24 * half * units - (0 if half > 64 else 2 * MIB)
    args = (
        *own,
        *other,
        gate_matrix,
        pltpu.with_memory_space_constraint(up_matrix, pltpu.HBM),
        pltpu.with_memory_space_constraint(down_matrix, pltpu.HBM),
    )
    return call(
        lambda *refs: expert_kernel(layer, count, *refs),
        (shape(half, width), shape(half, width)),
        args,
        [VMEM] * (2 * count + 1) + [ANY] * 2,
        limit,
        scratch,
        12 * half * width * units,
    )


def exchange(near, far):
    devices = lax.axis_size("expert")
    split = devices // E_WIN
    if devices <= DIRECT:
        blocks = [near]
        for step in range(1, devices):
            pairs = [(i, i ^ step) for i in range(devices)]
            blocks.append(lax.ppermute(near if step < split else far, "expert", pairs))
        return blocks
    low = lax.axis_index("expert") < split
    first, second = jnp.where(low, near, far), jnp.where(low, far, near)
    outgoing = jnp.concatenate([jnp.repeat(first, split, axis=0), jnp.repeat(second, split, axis=0)])
    return [lax.all_to_all(outgoing, "expert", 0, 0, tiled=True)]


def give_back(blocks):
    devices = lax.axis_size("expert")
    if devices <= DIRECT:
        result = [blocks[0]]
        for step in range(1, devices):
            pairs = [(i, i ^ step) for i in range(devices)]
            result.append(lax.ppermute(blocks[step], "expert", pairs))
        return result
    split = devices // E_WIN
    returned = lax.all_to_all(blocks[0], "expert", 0, 0, tiled=True)
    turned = jnp.roll(returned, split, axis=0)
    return [jnp.where(lax.axis_index("expert") < split, returned, turned)]


def body(tokens, expert_ids, norm_gain, router, w_gate, w_up, w_down):
    layers = lax.axis_size("section")
    width = tokens.shape[-1]
    rows = tokens.shape[1]
    ids_own, gain_own, router_own = expert_ids[0], norm_gain, router[0].T
    params = (ids_own, swap(ids_own), gain_own, swap(gain_own), router_own, swap(router_own))
    slots = (shape(1, CAP, width), shape(1, CAP, width), shape(rows, E_WIN * CAP, dtype=f32))
    near, far, weights = call(first_kernel, slots, (tokens, *params), flops=10**10)
    stream = tokens
    for layer in range(layers):
        own = exchange(near, far)
        other = [swap(block) for block in own]
        own_terms, other_terms = experts(layer, own, other, w_gate[0], w_up[0], w_down[0])
        crossed = swap(other_terms)
        count = len(own)
        extra = 24 * CAP * sum(block.shape[0] for block in own) * width
        chosen = call(
            lambda *refs, layer=layer: select_kernel(layer, *refs),
            [shape(*block.shape) for block in own],
            (own_terms, crossed),
            limit=2 * MIB + extra // 2,
        )
        returned = give_back(chosen)
        if layer < layers - 1:
            stream, near, far, weights = call(
                lambda *refs, layer=layer: middle_kernel(count, layer + 1, *refs),
                (shape(rows, width), *slots),
                (stream, *returned, weights, *params),
                limit=2 * MIB + extra // 2,
                flops=10**12,
            )
        else:
            return call(
                lambda *refs: final_kernel(count, *refs),
                shape(1, rows, width),
                (stream, *returned, weights),
                limit=2 * MIB + extra // 2,
            )


def solution(mesh):
    in_specs = (
        P(None, ("groups", "expert"), None),
        P("section", None, ("groups", "expert"), None),
        P("section", None),
        P("section", None, None),
        P("section", None, "expert"),
        P("section", None, "expert"),
        P("section", "expert", None),
    )
    out_specs = P("section", ("groups", "expert"), None)
    return jax.shard_map(body, mesh=mesh, in_specs=in_specs, out_specs=out_specs, check_vma=False)
```

```python
import jax
import jax.numpy as jnp
from jax import lax
from jax.experimental import pallas as pl
from jax.experimental.pallas import tpu as pltpu
from jax.sharding import PartitionSpec as P

NEXP = 8
E_WIN = 2
CAP = 4
MIB = 1 << 20
DIRECT = 8


epsilon = 1e-05

VMEM = pl.BlockSpec(memory_space=pltpu.VMEM)
ANY = pl.BlockSpec(memory_space=pl.ANY)
f32 = jnp.float32
bf16 = jnp.bfloat16


def swap(value):
    count = lax.axis_size("section")
    return lax.ppermute(value, "section", [(s, (s + 1) % count) for s in range(count)])


def prepare(values, layer, ids_own, ids_other, gain_own, gain_other, router_own, router_other, near_ref, far_ref, weights_ref):
    section = lax.axis_index("section")
    split = lax.axis_size("expert") // E_WIN
    near = lax.axis_index("expert") // split
    mine = section == layer
    gain = jnp.where(mine, gain_own[...].astype(f32), gain_other[...].astype(f32))
    router = jnp.where(mine, router_own[...].astype(f32), router_other[...].astype(f32)).astype(bf16)
    ids = jnp.where(mine, ids_own[section], ids_other[section])
    scale = lax.rsqrt(jnp.mean(values * values, axis=-1, keepdims=True) + epsilon)
    normed = (values * scale * gain).astype(bf16)
    logits = lax.dot_general(normed, router, (((1,), (1,)), ((), ())), preferred_element_type=f32)
    tokens = values.shape[0]
    expert = lax.broadcasted_iota(jnp.int32, (tokens, NEXP), 1)
    first = (ids[:, 0:1] == expert).astype(f32)
    second = (ids[:, 1:2] == expert).astype(f32)
    chosen_first = jnp.sum(first * logits, axis=-1, keepdims=True)
    chosen_second = jnp.sum(second * logits, axis=-1, keepdims=True)
    gate_first = jax.nn.sigmoid(chosen_first - chosen_second)
    gate_second = jax.nn.sigmoid(chosen_second - chosen_first)
    named = first + second
    gates = first * gate_first + second * gate_second
    row = lax.broadcasted_iota(jnp.int32, (tokens, tokens), 0)
    column = lax.broadcasted_iota(jnp.int32, (tokens, tokens), 1)
    earlier = jnp.dot((column < row).astype(f32), named, preferred_element_type=f32)
    lane = lax.broadcasted_iota(jnp.int32, (tokens, E_WIN * CAP), 1)
    is_near = lane < CAP
    slot = jnp.where(is_near, lane, lane - CAP).astype(f32)

    def spread(table):
        low, high = table[:, 0:1], table[:, 1:2]
        return jnp.where(is_near == (near == 0), low, high)

    pick = spread(named) * (spread(earlier) == slot).astype(f32)
    weights_ref[...] = spread(gates) * pick
    packed = lax.dot_general(
        pick.astype(bf16), normed, (((0,), (0,)), ((), ())), preferred_element_type=f32
    )
    near_ref[0] = packed[:CAP].astype(bf16)
    far_ref[0] = packed[CAP:].astype(bf16)


def combine(values, weights_ref, returned):
    split = lax.axis_size("expert") // E_WIN
    blocks = [ref[index].astype(f32) for ref in returned for index in range(ref.shape[0])]
    result = values
    for side, group in enumerate((blocks[:split], blocks[split:])):
        total = group[0]
        for block in group[1:]:
            total = total + block
        for slot in range(CAP):
            column = side * CAP + slot
            result = result + weights_ref[:, column:column + 1] * total[slot:slot + 1, :]
    return result.astype(bf16)


def add_kernel(*refs):
    total = refs[0][...].astype(f32)
    for ref in refs[1:-1]:
        total = total + ref[...].astype(f32)
    refs[-1][...] = total.astype(bf16)


def first_kernel(tokens, ids_own, ids_other, gain_own, gain_other, router_own, router_other, *refs):
    outs, (stream, gain, router, sems) = refs[:3], refs[3:]
    copies = [
        pltpu.make_async_copy(tokens.at[lax.axis_index("section")], stream, sems.at[0]),
        pltpu.make_async_copy(gain_own, gain, sems.at[1]),
        pltpu.make_async_copy(router_own, router, sems.at[2]),
    ]
    for copy in copies:
        copy.start()
    for copy in copies:
        copy.wait()
    prepare(
        stream[...].astype(f32), 0, ids_own, ids_other, gain, gain_other, router, router_other, *outs
    )


def middle_kernel(count, layer, tokens, *refs):
    returned, refs = refs[:count], refs[count:]
    weights, refs = refs[0], refs[1:]
    params, outs = refs[:6], refs[6:]
    stream = combine(tokens[lax.axis_index("section")].astype(f32), weights, returned)
    outs[0][...] = stream
    prepare(stream.astype(f32), layer, *params, *outs[1:])


def final_kernel(count, stream, *refs):
    returned, weights, out = refs[:count], refs[count], refs[count + 1]
    out[0] = combine(stream[...].astype(f32), weights, returned)


def select_kernel(layer, own, crossed, *outs):
    mine = lax.axis_index("section") == layer
    row = 0
    pieces = [(out, index) for out in outs for index in range(out.shape[0])]
    for low in range(0, len(pieces), 2):
        lines = pl.ds(low * CAP, 2 * CAP)
        value = jnp.where(mine, own[lines, :].astype(f32), crossed[lines, :].astype(f32))
        for at, (out, index) in enumerate(pieces[low:low + 2]):
            out[index] = value[at * CAP:(at + 1) * CAP].astype(bf16)


def expert_kernel(layer, count, *refs):
    inputs, refs = refs[:2 * count], refs[2 * count:]
    gate_ref, up_hbm, down_hbm, own_out, other_out = refs[:5]
    rows_ref, up_buf, down_buf, gate_sum, up_sum, hidden_ref, total, up_sems, down_sems = refs[5:]
    half, width = own_out.shape
    units = gate_ref.shape[1]
    up_slots, depth, _ = up_buf.shape
    down_slots, block, _ = down_buf.shape
    steps, blocks = width // depth, units // block
    strip = width // 8

    def fetch_up(index, slot):
        lines = pl.ds(pl.multiple_of(index * depth, depth), depth)
        return pltpu.make_async_copy(up_hbm.at[lines], up_buf.at[slot], up_sems.at[slot])

    def fetch_down(index):
        slot = index % down_slots
        return pltpu.make_async_copy(
            down_hbm.at[pl.ds(index * block, block)], down_buf.at[slot], down_sems.at[slot]
        )

    for slot in range(up_slots):
        fetch_up(slot, slot).start()
    places = [(ref, index) for ref in inputs for index in range(ref.shape[0])]
    for low in range(0, len(places), 2):
        pair = [ref[index].astype(f32) for ref, index in places[low:low + 2]]
        rows_ref[pl.ds(low * CAP, 2 * CAP), :] = jnp.concatenate(pair, axis=0).astype(bf16)
    gate_sum[...] = jnp.zeros_like(gate_sum)
    up_sum[...] = jnp.zeros_like(up_sum)

    def enter(index, slot):
        lines = pl.ds(pl.multiple_of(index * depth, depth), depth)
        rows = rows_ref[:, lines]
        gate_sum[...] += jnp.dot(rows, gate_ref[lines, :], preferred_element_type=f32)
        fetch_up(index, slot).wait()
        up_sum[...] += jnp.dot(rows, up_buf[slot], preferred_element_type=f32)

    turns = steps // up_slots

    @pl.loop(0, turns - 1)
    def _(turn):
        for slot in range(up_slots):
            enter(turn * up_slots + slot, slot)
            fetch_up((turn + 1) * up_slots + slot, slot).start()

    for index in range(min(down_slots, blocks)):
        fetch_down(index).start()
    for slot in range(up_slots):
        enter((turns - 1) * up_slots + slot, slot)
    hidden_ref[...] = (jax.nn.silu(gate_sum[...]) * up_sum[...]).astype(bf16)

    for index in range(blocks):
        fetch_down(index).wait()
        hidden = hidden_ref[:, pl.ds(index * block, block)]
        for start in range(0, width, strip):
            columns = pl.ds(start, strip)
            value = jnp.dot(
                hidden, down_buf[index % down_slots, :, columns], preferred_element_type=f32
            )
            if index > 0:
                value += total[:, columns]
            if index == blocks - 1:
                value = value.astype(bf16)
                own_out[:, columns] = value[:half]
                other_out[:, columns] = value[half:]
            else:
                total[:, columns] = value
        if index + down_slots < blocks:
            fetch_down(index + down_slots).start()


def call(kernel, outs, args, specs=None, limit=2 * MIB, scratch=(), flops=10**6):
    many = isinstance(outs, (tuple, list))
    return pl.pallas_call(
        kernel,
        out_shape=tuple(outs) if many else outs,
        in_specs=specs or [VMEM] * len(args),
        out_specs=(VMEM,) * len(outs) if many else VMEM,
        scratch_shapes=list(scratch),
        compiler_params=pltpu.CompilerParams(vmem_limit_bytes=limit),
        cost_estimate=pl.CostEstimate(flops=flops, bytes_accessed=10**5, transcendentals=0),
    )(*args)


def shape(*sizes, dtype=bf16):
    return jax.ShapeDtypeStruct(sizes, dtype)


def experts(layer, own, other, gate_matrix, up_matrix, down_matrix):
    half = CAP * sum(block.shape[0] for block in own)
    width, units = gate_matrix.shape
    block = min(256, units)
    depth = width // 12
    up_slots, down_slots = 4, min(5, units // block)
    scratch = (
        pltpu.VMEM((2 * half, width), bf16),
        pltpu.VMEM((up_slots, depth, units), bf16),
        pltpu.VMEM((down_slots, block, width), bf16),
        pltpu.VMEM((2 * half, units), f32),
        pltpu.VMEM((2 * half, units), f32),
        pltpu.VMEM((2 * half, units), bf16),
        pltpu.VMEM((2 * half, width), f32),
        pltpu.SemaphoreType.DMA((up_slots,)),
        pltpu.SemaphoreType.DMA((down_slots,)),
    )
    count = len(own)
    limit = 2 * up_slots * depth * units + 2 * down_slots * block * width
    limit += 20 * half * width + 24 * half * units - (0 if half > 64 else 2 * MIB)
    args = (
        *own,
        *other,
        gate_matrix,
        pltpu.with_memory_space_constraint(up_matrix, pltpu.HBM),
        pltpu.with_memory_space_constraint(down_matrix, pltpu.HBM),
    )
    return call(
        lambda *refs: expert_kernel(layer, count, *refs),
        (shape(half, width), shape(half, width)),
        args,
        [VMEM] * (2 * count + 1) + [ANY] * 2,
        limit,
        scratch,
        12 * half * width * units,
    )


def across(value, step):
    devices = lax.axis_size("expert")
    return lax.ppermute(value, "expert", [(i, i ^ step) for i in range(devices)])


def exchange(near, far):
    devices = lax.axis_size("expert")
    split = devices // E_WIN
    if devices <= DIRECT:
        cross = across(far, split)
        return [
            block if step == 0 else across(block, step)
            for block in (near, cross)
            for step in range(split)
        ]
    low = lax.axis_index("expert") < split
    first, second = jnp.where(low, near, far), jnp.where(low, far, near)
    outgoing = jnp.concatenate([jnp.repeat(first, split, axis=0), jnp.repeat(second, split, axis=0)])
    return [lax.all_to_all(outgoing, "expert", 0, 0, tiled=True)]


def give_back(blocks):
    devices = lax.axis_size("expert")
    split = devices // E_WIN
    if devices <= DIRECT:
        far = [blocks[split]] + [across(blocks[split + step], step) for step in range(1, split)]
        near = [blocks[0]] + [across(blocks[step], step) for step in range(1, split)]
        total = call(add_kernel, shape(*far[0].shape), far)
        return near + [across(total, split)]
    returned = lax.all_to_all(blocks[0], "expert", 0, 0, tiled=True)
    turned = jnp.roll(returned, split, axis=0)
    return [jnp.where(lax.axis_index("expert") < split, returned, turned)]


def body(tokens, expert_ids, norm_gain, router, w_gate, w_up, w_down):
    layers = lax.axis_size("section")
    width = tokens.shape[-1]
    rows = tokens.shape[1]
    ids_own, gain_own, router_own = expert_ids[0], norm_gain, router[0].T
    params = (ids_own, swap(ids_own), gain_own, swap(gain_own), router_own, swap(router_own))
    slots = (shape(1, CAP, width), shape(1, CAP, width), shape(rows, E_WIN * CAP, dtype=f32))
    hbm = [pltpu.with_memory_space_constraint(x, pltpu.HBM) for x in (tokens, gain_own, router_own)]
    near, far, weights = call(
        first_kernel,
        slots,
        (hbm[0], *params[:2], hbm[1], params[3], hbm[2], params[5]),
        [ANY, VMEM, VMEM, ANY, VMEM, ANY, VMEM],
        scratch=[
            pltpu.VMEM((rows, width), bf16),
            pltpu.VMEM(gain_own.shape, bf16),
            pltpu.VMEM(router_own.shape, bf16),
            pltpu.SemaphoreType.DMA((3,)),
        ],
        flops=10**10,
    )
    stream = tokens
    for layer in range(layers):
        own = exchange(near, far)
        other = [swap(block) for block in own]
        own_terms, other_terms = experts(layer, own, other, w_gate[0], w_up[0], w_down[0])
        crossed = swap(other_terms)
        count = len(own)
        extra = 24 * CAP * sum(block.shape[0] for block in own) * width
        chosen = call(
            lambda *refs, layer=layer: select_kernel(layer, *refs),
            [shape(*block.shape) for block in own],
            (own_terms, crossed),
            limit=2 * MIB + extra // 2,
        )
        returned = give_back(chosen)
        count = len(returned)
        if layer < layers - 1:
            stream, near, far, weights = call(
                lambda *refs, layer=layer: middle_kernel(count, layer + 1, *refs),
                (shape(rows, width), *slots),
                (stream, *returned, weights, *params),
                limit=2 * MIB + extra // 2,
                flops=10**12,
            )
        else:
            return call(
                lambda *refs: final_kernel(count, *refs),
                shape(1, rows, width),
                (stream, *returned, weights),
                limit=2 * MIB + extra // 2,
            )


def solution(mesh):
    in_specs = (
        P(None, ("groups", "expert"), None),
        P("section", None, ("groups", "expert"), None),
        P("section", None),
        P("section", None, None),
        P("section", None, "expert"),
        P("section", None, "expert"),
        P("section", "expert", None),
    )
    out_specs = P("section", ("groups", "expert"), None)
    return jax.shard_map(body, mesh=mesh, in_specs=in_specs, out_specs=out_specs, check_vma=False)
```

```python
import jax
import jax.numpy as jnp
from jax import lax
from jax.experimental import pallas as pl
from jax.experimental.pallas import tpu as pltpu
from jax.sharding import PartitionSpec as P

NEXP = 8
E_WIN = 2
CAP = 4
MIB = 1 << 20
DIRECT = 8


epsilon = 1e-05

VMEM = pl.BlockSpec(memory_space=pltpu.VMEM)
ANY = pl.BlockSpec(memory_space=pl.ANY)
f32 = jnp.float32
bf16 = jnp.bfloat16


def swap(value):
    count = lax.axis_size("section")
    return lax.ppermute(value, "section", [(s, (s + 1) % count) for s in range(count)])


def prepare(values, layer, ids_own, ids_other, gain_own, gain_other, router_own, router_other, near_ref, far_ref, weights_ref):
    section = lax.axis_index("section")
    split = lax.axis_size("expert") // E_WIN
    near = lax.axis_index("expert") // split
    mine = section == layer
    gain = jnp.where(mine, gain_own[...].astype(f32), gain_other[...].astype(f32))
    router = jnp.where(mine, router_own[...].astype(f32), router_other[...].astype(f32)).astype(bf16)
    ids = jnp.where(mine, ids_own[section], ids_other[section])
    scale = lax.rsqrt(jnp.mean(values * values, axis=-1, keepdims=True) + epsilon)
    normed = (values * scale * gain).astype(bf16)
    logits = lax.dot_general(normed, router, (((1,), (1,)), ((), ())), preferred_element_type=f32)
    tokens = values.shape[0]
    expert = lax.broadcasted_iota(jnp.int32, (tokens, NEXP), 1)
    first = (ids[:, 0:1] == expert).astype(f32)
    second = (ids[:, 1:2] == expert).astype(f32)
    chosen_first = jnp.sum(first * logits, axis=-1, keepdims=True)
    chosen_second = jnp.sum(second * logits, axis=-1, keepdims=True)
    gate_first = jax.nn.sigmoid(chosen_first - chosen_second)
    gate_second = jax.nn.sigmoid(chosen_second - chosen_first)
    named = first + second
    gates = first * gate_first + second * gate_second
    row = lax.broadcasted_iota(jnp.int32, (tokens, tokens), 0)
    column = lax.broadcasted_iota(jnp.int32, (tokens, tokens), 1)
    earlier = jnp.dot((column < row).astype(f32), named, preferred_element_type=f32)
    lane = lax.broadcasted_iota(jnp.int32, (tokens, E_WIN * CAP), 1)
    is_near = lane < CAP
    slot = jnp.where(is_near, lane, lane - CAP).astype(f32)

    def spread(table):
        low, high = table[:, 0:1], table[:, 1:2]
        return jnp.where(is_near == (near == 0), low, high)

    pick = spread(named) * (spread(earlier) == slot).astype(f32)
    weights_ref[...] = spread(gates) * pick
    packed = lax.dot_general(
        pick.astype(bf16), normed, (((0,), (0,)), ((), ())), preferred_element_type=f32
    )
    near_ref[0] = packed[:CAP].astype(bf16)
    far_ref[0] = packed[CAP:].astype(bf16)


def combine(values, weights_ref, returned):
    split = lax.axis_size("expert") // E_WIN
    blocks = [ref[index].astype(f32) for ref in returned for index in range(ref.shape[0])]
    result = values
    for side, group in enumerate((blocks[:split], blocks[split:])):
        total = group[0]
        for block in group[1:]:
            total = total + block
        for slot in range(CAP):
            column = side * CAP + slot
            result = result + weights_ref[:, column:column + 1] * total[slot:slot + 1, :]
    return result.astype(bf16)


def add_kernel(*refs):
    total = refs[0][...].astype(f32)
    for ref in refs[1:-1]:
        total = total + ref[...].astype(f32)
    refs[-1][...] = total.astype(bf16)


def first_kernel(tokens, ids_own, ids_other, gain_own, gain_other, router_own, router_other, *refs):
    outs, (stream, gain, router, sems) = refs[:3], refs[3:]
    copies = [
        pltpu.make_async_copy(tokens.at[lax.axis_index("section")], stream, sems.at[0]),
        pltpu.make_async_copy(gain_own, gain, sems.at[1]),
        pltpu.make_async_copy(router_own, router, sems.at[2]),
    ]
    for copy in copies:
        copy.start()
    for copy in copies:
        copy.wait()
    prepare(
        stream[...].astype(f32), 0, ids_own, ids_other, gain, gain_other, router, router_other, *outs
    )


def middle_kernel(count, layer, tokens, *refs):
    returned, refs = refs[:count], refs[count:]
    weights, refs = refs[0], refs[1:]
    params, outs = refs[:6], refs[6:]
    stream = combine(tokens[lax.axis_index("section")].astype(f32), weights, returned)
    outs[0][...] = stream
    prepare(stream.astype(f32), layer, *params, *outs[1:])


def final_kernel(count, stream, *refs):
    returned, weights, out = refs[:count], refs[count], refs[count + 1]
    out[0] = combine(stream[...].astype(f32), weights, returned)


def select_kernel(layer, own, crossed, *outs):
    mine = lax.axis_index("section") == layer
    row = 0
    pieces = [(out, index) for out in outs for index in range(out.shape[0])]
    for low in range(0, len(pieces), 2):
        lines = pl.ds(low * CAP, 2 * CAP)
        value = jnp.where(mine, own[lines, :].astype(f32), crossed[lines, :].astype(f32))
        for at, (out, index) in enumerate(pieces[low:low + 2]):
            out[index] = value[at * CAP:(at + 1) * CAP].astype(bf16)


def expert_kernel(layer, count, *refs):
    inputs, refs = refs[:2 * count], refs[2 * count:]
    gate_ref, held_ref, up_hbm, down_hbm, own_out, other_out = refs[:6]
    rows_ref, up_buf, down_buf, gate_sum, up_sum, hidden_ref, total, up_sems, down_sems = refs[6:]
    half, width = own_out.shape
    units = gate_ref.shape[1]
    held = held_ref.shape[0]
    up_slots, depth, _ = up_buf.shape
    down_slots, block, _ = down_buf.shape
    steps, blocks = (width - held) // depth, units // block
    strip = width // 8

    def fetch_up(index, slot):
        lines = pl.ds(pl.multiple_of(held + index * depth, depth), depth)
        return pltpu.make_async_copy(up_hbm.at[lines], up_buf.at[slot], up_sems.at[slot])

    def fetch_down(index):
        slot = index % down_slots
        return pltpu.make_async_copy(
            down_hbm.at[pl.ds(index * block, block)], down_buf.at[slot], down_sems.at[slot]
        )

    for slot in range(up_slots):
        fetch_up(slot, slot).start()
    places = [(ref, index) for ref in inputs for index in range(ref.shape[0])]
    for low in range(0, len(places), 2):
        pair = [ref[index].astype(f32) for ref, index in places[low:low + 2]]
        rows_ref[pl.ds(low * CAP, 2 * CAP), :] = jnp.concatenate(pair, axis=0).astype(bf16)
    gate_sum[...] = jnp.zeros_like(gate_sum)
    up_sum[...] = jnp.zeros_like(up_sum)

    def enter(index, slot):
        low = pl.ds(pl.multiple_of(index * depth, depth), depth)
        high = pl.ds(pl.multiple_of(held + index * depth, depth), depth)
        low_rows, high_rows = rows_ref[:, low], rows_ref[:, high]
        gate_sum[...] += jnp.dot(low_rows, gate_ref[low, :], preferred_element_type=f32)
        gate_sum[...] += jnp.dot(high_rows, gate_ref[high, :], preferred_element_type=f32)
        up_sum[...] += jnp.dot(low_rows, held_ref[low, :], preferred_element_type=f32)
        fetch_up(index, slot).wait()
        up_sum[...] += jnp.dot(high_rows, up_buf[slot], preferred_element_type=f32)

    turns = steps // up_slots

    @pl.loop(0, turns - 1)
    def _(turn):
        for slot in range(up_slots):
            enter(turn * up_slots + slot, slot)
            fetch_up((turn + 1) * up_slots + slot, slot).start()

    for index in range(min(down_slots, blocks)):
        fetch_down(index).start()
    for slot in range(up_slots):
        enter((turns - 1) * up_slots + slot, slot)
    hidden_ref[...] = (jax.nn.silu(gate_sum[...]) * up_sum[...]).astype(bf16)

    for index in range(blocks):
        fetch_down(index).wait()
        hidden = hidden_ref[:, pl.ds(index * block, block)]
        for start in range(0, width, strip):
            columns = pl.ds(start, strip)
            value = jnp.dot(
                hidden, down_buf[index % down_slots, :, columns], preferred_element_type=f32
            )
            if index > 0:
                value += total[:, columns]
            if index == blocks - 1:
                value = value.astype(bf16)
                own_out[:, columns] = value[:half]
                other_out[:, columns] = value[half:]
            else:
                total[:, columns] = value
        if index + down_slots < blocks:
            fetch_down(index + down_slots).start()


def load_kernel(source, after, target, sems):
    depth = target.shape[0] // sems.shape[0]
    copies = []
    for index in range(sems.shape[0]):
        lines = pl.ds(index * depth, depth)
        copies.append(pltpu.make_async_copy(source.at[lines], target.at[lines], sems.at[index]))
    for copy in copies:
        copy.start()
    for copy in copies:
        copy.wait()


def load(matrix, after):
    return call(
        load_kernel,
        pltpu.VMEM((matrix.shape[0] // 2, matrix.shape[1]), matrix.dtype),
        [pltpu.with_memory_space_constraint(matrix, pltpu.HBM), after],
        [ANY, ANY],
        MIB,
        [pltpu.SemaphoreType.DMA((4,))],
        LOADF,
    )


LOADF = 10**9
US, DS = 2, 2


def call(kernel, outs, args, specs=None, limit=2 * MIB, scratch=(), flops=10**6):
    many = isinstance(outs, (tuple, list))
    return pl.pallas_call(
        kernel,
        out_shape=tuple(outs) if many else outs,
        in_specs=specs or [VMEM] * len(args),
        out_specs=(VMEM,) * len(outs) if many else VMEM,
        scratch_shapes=list(scratch),
        compiler_params=pltpu.CompilerParams(vmem_limit_bytes=limit),
        cost_estimate=pl.CostEstimate(flops=flops, bytes_accessed=10**5, transcendentals=0),
    )(*args)


def shape(*sizes, dtype=bf16):
    return jax.ShapeDtypeStruct(sizes, dtype)


def experts(layer, own, other, gate_matrix, held, up_matrix, down_matrix):
    half = CAP * sum(block.shape[0] for block in own)
    width, units = gate_matrix.shape
    block = min(256, units)
    depth = width // 12
    up_slots, down_slots = US, min(DS, units // block)
    scratch = (
        pltpu.VMEM((2 * half, width), bf16),
        pltpu.VMEM((up_slots, depth, units), bf16),
        pltpu.VMEM((down_slots, block, width), bf16),
        pltpu.VMEM((2 * half, units), f32),
        pltpu.VMEM((2 * half, units), f32),
        pltpu.VMEM((2 * half, units), bf16),
        pltpu.VMEM((2 * half, width), f32),
        pltpu.SemaphoreType.DMA((up_slots,)),
        pltpu.SemaphoreType.DMA((down_slots,)),
    )
    count = len(own)
    limit = 2 * up_slots * depth * units + 2 * down_slots * block * width
    limit += 20 * half * width + 24 * half * units - (0 if half > 64 else -MIB)
    args = (
        *own,
        *other,
        gate_matrix,
        pltpu.with_memory_space_constraint(held, pltpu.VMEM),
        pltpu.with_memory_space_constraint(up_matrix, pltpu.HBM),
        pltpu.with_memory_space_constraint(down_matrix, pltpu.HBM),
    )
    return call(
        lambda *refs: expert_kernel(layer, count, *refs),
        (shape(half, width), shape(half, width)),
        args,
        [VMEM] * (2 * count + 2) + [ANY] * 2,
        limit,
        scratch,
        12 * half * width * units,
    )


def across(value, step):
    devices = lax.axis_size("expert")
    return lax.ppermute(value, "expert", [(i, i ^ step) for i in range(devices)])


def exchange(near, far):
    devices = lax.axis_size("expert")
    split = devices // E_WIN
    if devices <= DIRECT:
        cross = across(far, split)
        return [
            block if step == 0 else across(block, step)
            for block in (near, cross)
            for step in range(split)
        ]
    low = lax.axis_index("expert") < split
    first, second = jnp.where(low, near, far), jnp.where(low, far, near)
    outgoing = jnp.concatenate([jnp.repeat(first, split, axis=0), jnp.repeat(second, split, axis=0)])
    return [lax.all_to_all(outgoing, "expert", 0, 0, tiled=True)]


def give_back(blocks):
    devices = lax.axis_size("expert")
    split = devices // E_WIN
    if devices <= DIRECT:
        far = [blocks[split]] + [across(blocks[split + step], step) for step in range(1, split)]
        near = [blocks[0]] + [across(blocks[step], step) for step in range(1, split)]
        total = call(add_kernel, shape(*far[0].shape), far)
        return near + [across(total, split)]
    returned = lax.all_to_all(blocks[0], "expert", 0, 0, tiled=True)
    turned = jnp.roll(returned, split, axis=0)
    return [jnp.where(lax.axis_index("expert") < split, returned, turned)]


def body(tokens, expert_ids, norm_gain, router, w_gate, w_up, w_down):
    layers = lax.axis_size("section")
    split = min(DIRECT, lax.axis_size("expert")) // E_WIN if lax.axis_size("expert") <= DIRECT else 1
    width = tokens.shape[-1]
    rows = tokens.shape[1]
    ids_own, gain_own, router_own = expert_ids[0], norm_gain, router[0].T
    params = (ids_own, swap(ids_own), gain_own, swap(gain_own), router_own, swap(router_own))
    slots = (shape(1, CAP, width), shape(1, CAP, width), shape(rows, E_WIN * CAP, dtype=f32))
    hbm = [pltpu.with_memory_space_constraint(x, pltpu.HBM) for x in (tokens, gain_own, router_own)]
    near, far, weights = call(
        first_kernel,
        slots,
        (hbm[0], *params[:2], hbm[1], params[3], hbm[2], params[5]),
        [ANY, VMEM, VMEM, ANY, VMEM, ANY, VMEM],
        scratch=[
            pltpu.VMEM((rows, width), bf16),
            pltpu.VMEM(gain_own.shape, bf16),
            pltpu.VMEM(router_own.shape, bf16),
            pltpu.SemaphoreType.DMA((3,)),
        ],
        flops=10**12,
    )
    stream = tokens
    for layer in range(layers):
        own = exchange(near, far)
        other = [swap(block) for block in own]
        held = load(w_up[0], own[split - 1])
        own_terms, other_terms = experts(layer, own, other, w_gate[0], held, w_up[0], w_down[0])
        crossed = swap(other_terms)
        count = len(own)
        extra = 24 * CAP * sum(block.shape[0] for block in own) * width
        chosen = call(
            lambda *refs, layer=layer: select_kernel(layer, *refs),
            [shape(*block.shape) for block in own],
            (own_terms, crossed),
            limit=2 * MIB + extra // 2,
        )
        returned = give_back(chosen)
        count = len(returned)
        if layer < layers - 1:
            stream, near, far, weights = call(
                lambda *refs, layer=layer: middle_kernel(count, layer + 1, *refs),
                (shape(rows, width), *slots),
                (stream, *returned, weights, *params),
                limit=2 * MIB + extra // 2,
                flops=10**12,
            )
        else:
            return call(
                lambda *refs: final_kernel(count, *refs),
                shape(1, rows, width),
                (stream, *returned, weights),
                limit=2 * MIB + extra // 2,
            )


def solution(mesh):
    in_specs = (
        P(None, ("groups", "expert"), None),
        P("section", None, ("groups", "expert"), None),
        P("section", None),
        P("section", None, None),
        P("section", None, "expert"),
        P("section", None, "expert"),
        P("section", "expert", None),
    )
    out_specs = P("section", ("groups", "expert"), None)
    return jax.shard_map(body, mesh=mesh, in_specs=in_specs, out_specs=out_specs, check_vma=False)
```

```python
import jax
import jax.numpy as jnp
from jax import lax
from jax.experimental import pallas as pl
from jax.experimental.pallas import tpu as pltpu
from jax.sharding import PartitionSpec as P

NEXP = 8
E_WIN = 2
CAP = 4
MIB = 1 << 20
DIRECT = 8


epsilon = 1e-05

VMEM = pl.BlockSpec(memory_space=pltpu.VMEM)
ANY = pl.BlockSpec(memory_space=pl.ANY)
f32 = jnp.float32
bf16 = jnp.bfloat16


def swap(value):
    count = lax.axis_size("section")
    return lax.ppermute(value, "section", [(s, (s + 1) % count) for s in range(count)])


def prepare(values, layer, ids_own, ids_other, gain_own, gain_other, router_own, router_other, near_ref, far_ref, weights_ref):
    section = lax.axis_index("section")
    split = lax.axis_size("expert") // E_WIN
    near = lax.axis_index("expert") // split
    mine = section == layer
    gain = jnp.where(mine, gain_own[...].astype(f32), gain_other[...].astype(f32))
    router = jnp.where(mine, router_own[...].astype(f32), router_other[...].astype(f32)).astype(bf16)
    ids = jnp.where(mine, ids_own[section], ids_other[section])
    scale = lax.rsqrt(jnp.mean(values * values, axis=-1, keepdims=True) + epsilon)
    normed = (values * scale * gain).astype(bf16)
    logits = lax.dot_general(normed, router, (((1,), (1,)), ((), ())), preferred_element_type=f32)
    tokens = values.shape[0]
    expert = lax.broadcasted_iota(jnp.int32, (tokens, NEXP), 1)
    first = (ids[:, 0:1] == expert).astype(f32)
    second = (ids[:, 1:2] == expert).astype(f32)
    chosen_first = jnp.sum(first * logits, axis=-1, keepdims=True)
    chosen_second = jnp.sum(second * logits, axis=-1, keepdims=True)
    gate_first = jax.nn.sigmoid(chosen_first - chosen_second)
    gate_second = jax.nn.sigmoid(chosen_second - chosen_first)
    named = first + second
    gates = first * gate_first + second * gate_second
    row = lax.broadcasted_iota(jnp.int32, (tokens, tokens), 0)
    column = lax.broadcasted_iota(jnp.int32, (tokens, tokens), 1)
    earlier = jnp.dot((column < row).astype(f32), named, preferred_element_type=f32)
    lane = lax.broadcasted_iota(jnp.int32, (tokens, E_WIN * CAP), 1)
    is_near = lane < CAP
    slot = jnp.where(is_near, lane, lane - CAP).astype(f32)

    def spread(table):
        low, high = table[:, 0:1], table[:, 1:2]
        return jnp.where(is_near == (near == 0), low, high)

    pick = spread(named) * (spread(earlier) == slot).astype(f32)
    weights_ref[...] = spread(gates) * pick
    packed = lax.dot_general(
        pick.astype(bf16), normed, (((0,), (0,)), ((), ())), preferred_element_type=f32
    )
    near_ref[0] = packed[:CAP].astype(bf16)
    far_ref[0] = packed[CAP:].astype(bf16)


def combine(values, weights_ref, returned):
    split = lax.axis_size("expert") // E_WIN
    blocks = [ref[index].astype(f32) for ref in returned for index in range(ref.shape[0])]
    result = values
    for side, group in enumerate((blocks[:split], blocks[split:])):
        total = group[0]
        for block in group[1:]:
            total = total + block
        for slot in range(CAP):
            column = side * CAP + slot
            result = result + weights_ref[:, column:column + 1] * total[slot:slot + 1, :]
    return result.astype(bf16)


def add_kernel(*refs):
    total = refs[0][...].astype(f32)
    for ref in refs[1:-1]:
        total = total + ref[...].astype(f32)
    refs[-1][...] = total.astype(bf16)


def first_kernel(tokens, ids_own, ids_other, gain_own, gain_other, router_own, router_other, *refs):
    outs, (stream, gain, router, sems) = refs[:3], refs[3:]
    copies = [
        pltpu.make_async_copy(tokens.at[lax.axis_index("section")], stream, sems.at[0]),
        pltpu.make_async_copy(gain_own, gain, sems.at[1]),
        pltpu.make_async_copy(router_own, router, sems.at[2]),
    ]
    for copy in copies:
        copy.start()
    for copy in copies:
        copy.wait()
    prepare(
        stream[...].astype(f32), 0, ids_own, ids_other, gain, gain_other, router, router_other, *outs
    )


def middle_kernel(count, layer, tokens, *refs):
    returned, refs = refs[:count], refs[count:]
    weights, refs = refs[0], refs[1:]
    params, outs = refs[:6], refs[6:]
    stream = combine(tokens[lax.axis_index("section")].astype(f32), weights, returned)
    outs[0][...] = stream
    prepare(stream.astype(f32), layer, *params, *outs[1:])


def final_kernel(count, stream, *refs):
    returned, weights, out = refs[:count], refs[count], refs[count + 1]
    out[0] = combine(stream[...].astype(f32), weights, returned)


def select_kernel(layer, own, crossed, *outs):
    mine = lax.axis_index("section") == layer
    row = 0
    pieces = [(out, index) for out in outs for index in range(out.shape[0])]
    for low in range(0, len(pieces), 2):
        lines = pl.ds(low * CAP, 2 * CAP)
        value = jnp.where(mine, own[lines, :].astype(f32), crossed[lines, :].astype(f32))
        for at, (out, index) in enumerate(pieces[low:low + 2]):
            out[index] = value[at * CAP:(at + 1) * CAP].astype(bf16)


def expert_kernel(layer, count, *refs):
    inputs, refs = refs[:2 * count], refs[2 * count:]
    gate_ref, up_hbm, down_hbm, own_out, other_out = refs[:5]
    rows_ref, up_buf, down_buf, gate_sum, up_sum, hidden_ref, total, up_sems, down_sems = refs[5:]
    half, width = own_out.shape
    real, padded = 2 * half, rows_ref.shape[0]
    units = gate_ref.shape[1]
    up_slots, depth, _ = up_buf.shape
    down_slots, block, _ = down_buf.shape
    steps, blocks = width // depth, units // block
    strip = width // 8

    def fetch_up(index, slot):
        lines = pl.ds(pl.multiple_of(index * depth, depth), depth)
        return pltpu.make_async_copy(up_hbm.at[lines], up_buf.at[slot], up_sems.at[slot])

    def fetch_down(index):
        slot = index % down_slots
        return pltpu.make_async_copy(
            down_hbm.at[pl.ds(index * block, block)], down_buf.at[slot], down_sems.at[slot]
        )

    for slot in range(up_slots):
        fetch_up(slot, slot).start()
    places = [(ref, index) for ref in inputs for index in range(ref.shape[0])]
    for low in range(0, len(places), 2):
        pair = [ref[index].astype(f32) for ref, index in places[low:low + 2]]
        lines = jnp.concatenate(pair, axis=0).astype(bf16)
        for start in range(0, padded, real):
            rows_ref[pl.ds(start + low * CAP, 2 * CAP), :] = lines

    def gate_part(index, fresh=False):
        lines = pl.ds(pl.multiple_of(index * depth, depth), depth)
        value = jnp.dot(rows_ref[:, lines], gate_ref[lines, :], preferred_element_type=f32)[:real]
        gate_sum[...] = value if fresh else gate_sum[...] + value

    def up_part(index, slot):
        lines = pl.ds(pl.multiple_of(index * depth, depth), depth)
        value = jnp.dot(rows_ref[:, lines], up_buf[slot], preferred_element_type=f32)[:real]
        up_sum[...] += value

    up_sum[...] = jnp.zeros_like(up_sum)
    gate_part(0, True)
    turns = steps // up_slots

    def turn_of(turn, last):
        for slot in range(up_slots):
            index = turn * up_slots + slot
            fetch_up(index, slot).wait()
            up_part(index, slot)
            if not (last and slot == up_slots - 1):
                gate_part(index + 1)
            if not last:
                fetch_up(index + up_slots, slot).start()

    @pl.loop(0, turns - 1)
    def _(turn):
        turn_of(turn, False)

    for index in range(min(down_slots, blocks)):
        fetch_down(index).start()
    turn_of(turns - 1, True)
    for start in range(0, padded, real):
        hidden_ref[start:start + real, :] = (
            jax.nn.silu(gate_sum[...]) * up_sum[...]
        ).astype(bf16)

    for index in range(blocks):
        fetch_down(index).wait()
        hidden = hidden_ref[:, pl.ds(index * block, block)]
        for start in range(0, width, strip):
            columns = pl.ds(start, strip)
            value = jnp.dot(
                hidden, down_buf[index % down_slots, :, columns], preferred_element_type=f32
            )[:real]
            if index > 0:
                value += total[:, columns]
            if index == blocks - 1:
                value = value.astype(bf16)
                own_out[:, columns] = value[:half]
                other_out[:, columns] = value[half:]
            else:
                total[:, columns] = value
        if index + down_slots < blocks:
            fetch_down(index + down_slots).start()


def call(kernel, outs, args, specs=None, limit=2 * MIB, scratch=(), flops=10**6):
    many = isinstance(outs, (tuple, list))
    return pl.pallas_call(
        kernel,
        out_shape=tuple(outs) if many else outs,
        in_specs=specs or [VMEM] * len(args),
        out_specs=(VMEM,) * len(outs) if many else VMEM,
        scratch_shapes=list(scratch),
        compiler_params=pltpu.CompilerParams(vmem_limit_bytes=limit),
        cost_estimate=pl.CostEstimate(flops=flops, bytes_accessed=10**5, transcendentals=0),
    )(*args)


def shape(*sizes, dtype=bf16):
    return jax.ShapeDtypeStruct(sizes, dtype)


def experts(layer, own, other, gate_matrix, up_matrix, down_matrix):
    half = CAP * sum(block.shape[0] for block in own)
    width, units = gate_matrix.shape
    block = min(256, units)
    depth = width // 12
    up_slots, down_slots = 4, min(5, units // block)
    padded = max(2 * half, 128)
    scratch = (
        pltpu.VMEM((padded, width), bf16),
        pltpu.VMEM((up_slots, depth, units), bf16),
        pltpu.VMEM((down_slots, block, width), bf16),
        pltpu.VMEM((2 * half, units), f32),
        pltpu.VMEM((2 * half, units), f32),
        pltpu.VMEM((padded, units), bf16),
        pltpu.VMEM((2 * half, width), f32),
        pltpu.SemaphoreType.DMA((up_slots,)),
        pltpu.SemaphoreType.DMA((down_slots,)),
    )
    count = len(own)
    limit = 2 * up_slots * depth * units + 2 * down_slots * block * width
    limit += 20 * half * width + 24 * half * units - (0 if half > 64 else 1 * MIB)
    args = (
        *own,
        *other,
        gate_matrix,
        pltpu.with_memory_space_constraint(up_matrix, pltpu.HBM),
        pltpu.with_memory_space_constraint(down_matrix, pltpu.HBM),
    )
    return call(
        lambda *refs: expert_kernel(layer, count, *refs),
        (shape(half, width), shape(half, width)),
        args,
        [VMEM] * (2 * count + 1) + [ANY] * 2,
        limit,
        scratch,
        12 * half * width * units,
    )


def across(value, step):
    devices = lax.axis_size("expert")
    return lax.ppermute(value, "expert", [(i, i ^ step) for i in range(devices)])


def exchange(near, far):
    devices = lax.axis_size("expert")
    split = devices // E_WIN
    if devices <= DIRECT:
        cross = across(far, split)
        return [
            block if step == 0 else across(block, step)
            for block in (near, cross)
            for step in range(split)
        ]
    low = lax.axis_index("expert") < split
    first, second = jnp.where(low, near, far), jnp.where(low, far, near)
    outgoing = jnp.concatenate([jnp.repeat(first, split, axis=0), jnp.repeat(second, split, axis=0)])
    return [lax.all_to_all(outgoing, "expert", 0, 0, tiled=True)]


def give_back(blocks):
    devices = lax.axis_size("expert")
    split = devices // E_WIN
    if devices <= DIRECT:
        far = [blocks[split]] + [across(blocks[split + step], step) for step in range(1, split)]
        near = [blocks[0]] + [across(blocks[step], step) for step in range(1, split)]
        total = call(add_kernel, shape(*far[0].shape), far)
        return near + [across(total, split)]
    returned = lax.all_to_all(blocks[0], "expert", 0, 0, tiled=True)
    turned = jnp.roll(returned, split, axis=0)
    return [jnp.where(lax.axis_index("expert") < split, returned, turned)]


def body(tokens, expert_ids, norm_gain, router, w_gate, w_up, w_down):
    layers = lax.axis_size("section")
    width = tokens.shape[-1]
    rows = tokens.shape[1]
    ids_own, gain_own, router_own = expert_ids[0], norm_gain, router[0].T
    params = (ids_own, swap(ids_own), gain_own, swap(gain_own), router_own, swap(router_own))
    slots = (shape(1, CAP, width), shape(1, CAP, width), shape(rows, E_WIN * CAP, dtype=f32))
    hbm = [pltpu.with_memory_space_constraint(x, pltpu.HBM) for x in (tokens, gain_own, router_own)]
    near, far, weights = call(
        first_kernel,
        slots,
        (hbm[0], *params[:2], hbm[1], params[3], hbm[2], params[5]),
        [ANY, VMEM, VMEM, ANY, VMEM, ANY, VMEM],
        scratch=[
            pltpu.VMEM((rows, width), bf16),
            pltpu.VMEM(gain_own.shape, bf16),
            pltpu.VMEM(router_own.shape, bf16),
            pltpu.SemaphoreType.DMA((3,)),
        ],
        flops=10**12,
    )
    stream = tokens
    for layer in range(layers):
        own = exchange(near, far)
        other = [swap(block) for block in own]
        own_terms, other_terms = experts(layer, own, other, w_gate[0], w_up[0], w_down[0])
        crossed = swap(other_terms)
        count = len(own)
        extra = 24 * CAP * sum(block.shape[0] for block in own) * width
        chosen = call(
            lambda *refs, layer=layer: select_kernel(layer, *refs),
            [shape(*block.shape) for block in own],
            (own_terms, crossed),
            limit=2 * MIB + extra // 2,
        )
        returned = give_back(chosen)
        count = len(returned)
        if layer < layers - 1:
            stream, near, far, weights = call(
                lambda *refs, layer=layer: middle_kernel(count, layer + 1, *refs),
                (shape(rows, width), *slots),
                (stream, *returned, weights, *params),
                limit=2 * MIB + extra // 2,
                flops=10**12,
            )
        else:
            return call(
                lambda *refs: final_kernel(count, *refs),
                shape(1, rows, width),
                (stream, *returned, weights),
                limit=2 * MIB + extra // 2,
            )


def solution(mesh):
    in_specs = (
        P(None, ("groups", "expert"), None),
        P("section", None, ("groups", "expert"), None),
        P("section", None),
        P("section", None, None),
        P("section", None, "expert"),
        P("section", None, "expert"),
        P("section", "expert", None),
    )
    out_specs = P("section", ("groups", "expert"), None)
    return jax.shard_map(body, mesh=mesh, in_specs=in_specs, out_specs=out_specs, check_vma=False)
```

```python
import jax
import jax.numpy as jnp
from jax import lax
from jax.experimental import pallas as pl
from jax.experimental.pallas import tpu as pltpu
from jax.sharding import PartitionSpec as P

NEXP = 8
E_WIN = 2
CAP = 4
MIB = 1 << 20
DIRECT = 8


epsilon = 1e-05

VMEM = pl.BlockSpec(memory_space=pltpu.VMEM)
ANY = pl.BlockSpec(memory_space=pl.ANY)
f32 = jnp.float32
bf16 = jnp.bfloat16


def swap(value):
    count = lax.axis_size("section")
    return lax.ppermute(value, "section", [(s, (s + 1) % count) for s in range(count)])


def prepare(values, layer, ids_own, ids_other, gain_own, gain_other, router_own, router_other, near_ref, far_ref, weights_ref):
    section = lax.axis_index("section")
    split = lax.axis_size("expert") // E_WIN
    near = lax.axis_index("expert") // split
    mine = section == layer
    gain = jnp.where(mine, gain_own[...].astype(f32), gain_other[...].astype(f32))
    router = jnp.where(mine, router_own[...].astype(f32), router_other[...].astype(f32)).astype(bf16)
    ids = jnp.where(mine, ids_own[section], ids_other[section])
    scale = lax.rsqrt(jnp.mean(values * values, axis=-1, keepdims=True) + epsilon)
    normed = (values * scale * gain).astype(bf16)
    logits = lax.dot_general(normed, router, (((1,), (1,)), ((), ())), preferred_element_type=f32)
    tokens = values.shape[0]
    expert = lax.broadcasted_iota(jnp.int32, (tokens, NEXP), 1)
    first = (ids[:, 0:1] == expert).astype(f32)
    second = (ids[:, 1:2] == expert).astype(f32)
    chosen_first = jnp.sum(first * logits, axis=-1, keepdims=True)
    chosen_second = jnp.sum(second * logits, axis=-1, keepdims=True)
    gate_first = jax.nn.sigmoid(chosen_first - chosen_second)
    gate_second = jax.nn.sigmoid(chosen_second - chosen_first)
    named = first + second
    gates = first * gate_first + second * gate_second
    row = lax.broadcasted_iota(jnp.int32, (tokens, tokens), 0)
    column = lax.broadcasted_iota(jnp.int32, (tokens, tokens), 1)
    earlier = jnp.dot((column < row).astype(f32), named, preferred_element_type=f32)
    lane = lax.broadcasted_iota(jnp.int32, (tokens, E_WIN * CAP), 1)
    is_near = lane < CAP
    slot = jnp.where(is_near, lane, lane - CAP).astype(f32)

    def spread(table):
        low, high = table[:, 0:1], table[:, 1:2]
        return jnp.where(is_near == (near == 0), low, high)

    pick = spread(named) * (spread(earlier) == slot).astype(f32)
    weights_ref[...] = spread(gates) * pick
    packed = lax.dot_general(
        pick.astype(bf16), normed, (((0,), (0,)), ((), ())), preferred_element_type=f32
    )
    near_ref[0] = packed[:CAP].astype(bf16)
    far_ref[0] = packed[CAP:].astype(bf16)


def combine(values, weights_ref, returned):
    split = lax.axis_size("expert") // E_WIN
    blocks = [ref[index].astype(f32) for ref in returned for index in range(ref.shape[0])]
    result = values
    for side, group in enumerate((blocks[:split], blocks[split:])):
        total = group[0]
        for block in group[1:]:
            total = total + block
        for slot in range(CAP):
            column = side * CAP + slot
            result = result + weights_ref[:, column:column + 1] * total[slot:slot + 1, :]
    return result.astype(bf16)


def add_kernel(*refs):
    total = refs[0][...].astype(f32)
    for ref in refs[1:-1]:
        total = total + ref[...].astype(f32)
    refs[-1][...] = total.astype(bf16)


def first_kernel(tokens, ids_own, ids_other, gain_own, gain_other, router_own, router_other, *refs):
    outs, (stream, gain, router, sems) = refs[:3], refs[3:]
    copies = [
        pltpu.make_async_copy(tokens.at[lax.axis_index("section")], stream, sems.at[0]),
        pltpu.make_async_copy(gain_own, gain, sems.at[1]),
        pltpu.make_async_copy(router_own, router, sems.at[2]),
    ]
    for copy in copies:
        copy.start()
    for copy in copies:
        copy.wait()
    prepare(
        stream[...].astype(f32), 0, ids_own, ids_other, gain, gain_other, router, router_other, *outs
    )


def middle_kernel(count, layer, tokens, *refs):
    returned, refs = refs[:count], refs[count:]
    weights, refs = refs[0], refs[1:]
    params, outs = refs[:6], refs[6:]
    stream = combine(tokens[lax.axis_index("section")].astype(f32), weights, returned)
    outs[0][...] = stream
    prepare(stream.astype(f32), layer, *params, *outs[1:])


def final_kernel(count, stream, *refs):
    returned, weights, out = refs[:count], refs[count], refs[count + 1]
    out[0] = combine(stream[...].astype(f32), weights, returned)


def select_kernel(layer, own, crossed, *outs):
    mine = lax.axis_index("section") == layer
    row = 0
    pieces = [(out, index) for out in outs for index in range(out.shape[0])]
    for low in range(0, len(pieces), 2):
        lines = pl.ds(low * CAP, 2 * CAP)
        value = jnp.where(mine, own[lines, :].astype(f32), crossed[lines, :].astype(f32))
        for at, (out, index) in enumerate(pieces[low:low + 2]):
            out[index] = value[at * CAP:(at + 1) * CAP].astype(bf16)


def expert_kernel(layer, count, *refs):
    inputs, refs = refs[:2 * count], refs[2 * count:]
    gate_ref, up_hbm, down_hbm, own_out, other_out = refs[:5]
    rows_ref, up_buf, down_buf, gate_sum, up_sum, hidden_ref, total, up_sems, down_sems = refs[5:]
    half, width = own_out.shape
    real, padded = 2 * half, rows_ref.shape[0]
    units = gate_ref.shape[1]
    up_slots, depth, _ = up_buf.shape
    down_slots, block, _ = down_buf.shape
    steps, blocks = width // depth, units // block
    strip = width // 8

    def fetch_up(index, slot):
        lines = pl.ds(pl.multiple_of(index * depth, depth), depth)
        return pltpu.make_async_copy(up_hbm.at[lines], up_buf.at[slot], up_sems.at[slot])

    def fetch_down(index):
        slot = index % down_slots
        return pltpu.make_async_copy(
            down_hbm.at[pl.ds(index * block, block)], down_buf.at[slot], down_sems.at[slot]
        )

    for slot in range(up_slots):
        fetch_up(slot, slot).start()
    for index in range(min(down_slots, blocks)):
        fetch_down(index).start(priority=1)
    places = [(ref, index) for ref in inputs for index in range(ref.shape[0])]
    for low in range(0, len(places), 2):
        pair = [ref[index].astype(f32) for ref, index in places[low:low + 2]]
        lines = jnp.concatenate(pair, axis=0).astype(bf16)
        for start in range(0, padded, real):
            rows_ref[pl.ds(start + low * CAP, 2 * CAP), :] = lines

    def gate_part(index, fresh=False):
        lines = pl.ds(pl.multiple_of(index * depth, depth), depth)
        value = jnp.dot(rows_ref[:, lines], gate_ref[lines, :], preferred_element_type=f32)[:real]
        gate_sum[...] = value if fresh else gate_sum[...] + value

    def up_part(index, slot):
        lines = pl.ds(pl.multiple_of(index * depth, depth), depth)
        value = jnp.dot(rows_ref[:, lines], up_buf[slot], preferred_element_type=f32)[:real]
        up_sum[...] += value

    up_sum[...] = jnp.zeros_like(up_sum)
    gate_part(0, True)
    turns = steps // up_slots

    def turn_of(turn, last):
        for slot in range(up_slots):
            index = turn * up_slots + slot
            fetch_up(index, slot).wait()
            up_part(index, slot)
            if not (last and slot == up_slots - 1):
                gate_part(index + 1)
            if not last:
                fetch_up(index + up_slots, slot).start()

    @pl.loop(0, turns - 1)
    def _(turn):
        turn_of(turn, False)

    turn_of(turns - 1, True)
    for start in range(0, padded, real):
        hidden_ref[start:start + real, :] = (
            jax.nn.silu(gate_sum[...]) * up_sum[...]
        ).astype(bf16)

    for index in range(blocks):
        fetch_down(index).wait()
        hidden = hidden_ref[:, pl.ds(index * block, block)]
        for start in range(0, width, strip):
            columns = pl.ds(start, strip)
            value = jnp.dot(
                hidden, down_buf[index % down_slots, :, columns], preferred_element_type=f32
            )[:real]
            if index > 0:
                value += total[:, columns]
            if index == blocks - 1:
                value = value.astype(bf16)
                own_out[:, columns] = value[:half]
                other_out[:, columns] = value[half:]
            else:
                total[:, columns] = value
        if index + down_slots < blocks:
            fetch_down(index + down_slots).start(priority=1)


def call(kernel, outs, args, specs=None, limit=2 * MIB, scratch=(), flops=10**6):
    many = isinstance(outs, (tuple, list))
    return pl.pallas_call(
        kernel,
        out_shape=tuple(outs) if many else outs,
        in_specs=specs or [VMEM] * len(args),
        out_specs=(VMEM,) * len(outs) if many else VMEM,
        scratch_shapes=list(scratch),
        compiler_params=pltpu.CompilerParams(vmem_limit_bytes=limit),
        cost_estimate=pl.CostEstimate(flops=flops, bytes_accessed=10**5, transcendentals=0),
    )(*args)


def shape(*sizes, dtype=bf16):
    return jax.ShapeDtypeStruct(sizes, dtype)


def experts(layer, own, other, gate_matrix, up_matrix, down_matrix):
    half = CAP * sum(block.shape[0] for block in own)
    width, units = gate_matrix.shape
    block = min(256, units)
    depth = width // 12
    up_slots, down_slots = 4, min(5, units // block)
    padded = max(2 * half, 128)
    scratch = (
        pltpu.VMEM((padded, width), bf16),
        pltpu.VMEM((up_slots, depth, units), bf16),
        pltpu.VMEM((down_slots, block, width), bf16),
        pltpu.VMEM((2 * half, units), f32),
        pltpu.VMEM((2 * half, units), f32),
        pltpu.VMEM((padded, units), bf16),
        pltpu.VMEM((2 * half, width), f32),
        pltpu.SemaphoreType.DMA((up_slots,)),
        pltpu.SemaphoreType.DMA((down_slots,)),
    )
    count = len(own)
    limit = 2 * up_slots * depth * units + 2 * down_slots * block * width
    limit += 20 * half * width + 24 * half * units - (0 if half > 64 else 1 * MIB)
    args = (
        *own,
        *other,
        gate_matrix,
        pltpu.with_memory_space_constraint(up_matrix, pltpu.HBM),
        pltpu.with_memory_space_constraint(down_matrix, pltpu.HBM),
    )
    return call(
        lambda *refs: expert_kernel(layer, count, *refs),
        (shape(half, width), shape(half, width)),
        args,
        [VMEM] * (2 * count + 1) + [ANY] * 2,
        limit,
        scratch,
        12 * half * width * units,
    )


def across(value, step):
    devices = lax.axis_size("expert")
    return lax.ppermute(value, "expert", [(i, i ^ step) for i in range(devices)])


def exchange(near, far):
    devices = lax.axis_size("expert")
    split = devices // E_WIN
    if devices <= DIRECT:
        cross = across(far, split)
        return [
            block if step == 0 else across(block, step)
            for block in (near, cross)
            for step in range(split)
        ]
    low = lax.axis_index("expert") < split
    first, second = jnp.where(low, near, far), jnp.where(low, far, near)
    outgoing = jnp.concatenate([jnp.repeat(first, split, axis=0), jnp.repeat(second, split, axis=0)])
    return [lax.all_to_all(outgoing, "expert", 0, 0, tiled=True)]


def give_back(blocks):
    devices = lax.axis_size("expert")
    split = devices // E_WIN
    if devices <= DIRECT:
        far = [blocks[split]] + [across(blocks[split + step], step) for step in range(1, split)]
        near = [blocks[0]] + [across(blocks[step], step) for step in range(1, split)]
        total = call(add_kernel, shape(*far[0].shape), far)
        return near + [across(total, split)]
    returned = lax.all_to_all(blocks[0], "expert", 0, 0, tiled=True)
    turned = jnp.roll(returned, split, axis=0)
    return [jnp.where(lax.axis_index("expert") < split, returned, turned)]


def body(tokens, expert_ids, norm_gain, router, w_gate, w_up, w_down):
    layers = lax.axis_size("section")
    width = tokens.shape[-1]
    rows = tokens.shape[1]
    ids_own, gain_own, router_own = expert_ids[0], norm_gain, router[0].T
    params = (ids_own, swap(ids_own), gain_own, swap(gain_own), router_own, swap(router_own))
    slots = (shape(1, CAP, width), shape(1, CAP, width), shape(rows, E_WIN * CAP, dtype=f32))
    hbm = [pltpu.with_memory_space_constraint(x, pltpu.HBM) for x in (tokens, gain_own, router_own)]
    near, far, weights = call(
        first_kernel,
        slots,
        (hbm[0], *params[:2], hbm[1], params[3], hbm[2], params[5]),
        [ANY, VMEM, VMEM, ANY, VMEM, ANY, VMEM],
        scratch=[
            pltpu.VMEM((rows, width), bf16),
            pltpu.VMEM(gain_own.shape, bf16),
            pltpu.VMEM(router_own.shape, bf16),
            pltpu.SemaphoreType.DMA((3,)),
        ],
        flops=10**12,
    )
    stream = tokens
    for layer in range(layers):
        own = exchange(near, far)
        other = [swap(block) for block in own]
        own_terms, other_terms = experts(layer, own, other, w_gate[0], w_up[0], w_down[0])
        crossed = swap(other_terms)
        count = len(own)
        extra = 24 * CAP * sum(block.shape[0] for block in own) * width
        chosen = call(
            lambda *refs, layer=layer: select_kernel(layer, *refs),
            [shape(*block.shape) for block in own],
            (own_terms, crossed),
            limit=2 * MIB + extra // 2,
        )
        returned = give_back(chosen)
        count = len(returned)
        if layer < layers - 1:
            stream, near, far, weights = call(
                lambda *refs, layer=layer: middle_kernel(count, layer + 1, *refs),
                (shape(rows, width), *slots),
                (stream, *returned, weights, *params),
                limit=2 * MIB + extra // 2,
                flops=10**12,
            )
        else:
            return call(
                lambda *refs: final_kernel(count, *refs),
                shape(1, rows, width),
                (stream, *returned, weights),
                limit=2 * MIB + extra // 2,
            )


def solution(mesh):
    in_specs = (
        P(None, ("groups", "expert"), None),
        P("section", None, ("groups", "expert"), None),
        P("section", None),
        P("section", None, None),
        P("section", None, "expert"),
        P("section", None, "expert"),
        P("section", "expert", None),
    )
    out_specs = P("section", ("groups", "expert"), None)
    return jax.shard_map(body, mesh=mesh, in_specs=in_specs, out_specs=out_specs, check_vma=False)
```

```python
import jax
import jax.numpy as jnp
from jax import lax
from jax.experimental import pallas as pl
from jax.experimental.pallas import tpu as pltpu
from jax.sharding import PartitionSpec as P

NEXP = 8
E_WIN = 2
CAP = 4
MIB = 1 << 20
DIRECT = 8


epsilon = 1e-05

VMEM = pl.BlockSpec(memory_space=pltpu.VMEM)
ANY = pl.BlockSpec(memory_space=pl.ANY)
f32 = jnp.float32
bf16 = jnp.bfloat16


def swap(value):
    count = lax.axis_size("section")
    return lax.ppermute(value, "section", [(s, (s + 1) % count) for s in range(count)])


def prepare(values, layer, ids_own, ids_other, gain_own, gain_other, router_own, router_other, near_ref, far_ref, weights_ref):
    section = lax.axis_index("section")
    split = lax.axis_size("expert") // E_WIN
    near = lax.axis_index("expert") // split
    mine = section == layer
    gain = jnp.where(mine, gain_own[...].astype(f32), gain_other[...].astype(f32))
    router = jnp.where(mine, router_own[...].astype(f32), router_other[...].astype(f32)).astype(bf16)
    ids = jnp.where(mine, ids_own[section], ids_other[section])
    scale = lax.rsqrt(jnp.mean(values * values, axis=-1, keepdims=True) + epsilon)
    normed = (values * scale * gain).astype(bf16)
    logits = lax.dot_general(normed, router, (((1,), (1,)), ((), ())), preferred_element_type=f32)
    tokens = values.shape[0]
    expert = lax.broadcasted_iota(jnp.int32, (tokens, NEXP), 1)
    first = (ids[:, 0:1] == expert).astype(f32)
    second = (ids[:, 1:2] == expert).astype(f32)
    chosen_first = jnp.sum(first * logits, axis=-1, keepdims=True)
    chosen_second = jnp.sum(second * logits, axis=-1, keepdims=True)
    gate_first = jax.nn.sigmoid(chosen_first - chosen_second)
    gate_second = jax.nn.sigmoid(chosen_second - chosen_first)
    named = first + second
    gates = first * gate_first + second * gate_second
    row = lax.broadcasted_iota(jnp.int32, (tokens, tokens), 0)
    column = lax.broadcasted_iota(jnp.int32, (tokens, tokens), 1)
    earlier = jnp.dot((column < row).astype(f32), named, preferred_element_type=f32)
    lane = lax.broadcasted_iota(jnp.int32, (tokens, E_WIN * CAP), 1)
    is_near = lane < CAP
    slot = jnp.where(is_near, lane, lane - CAP).astype(f32)

    def spread(table):
        low, high = table[:, 0:1], table[:, 1:2]
        return jnp.where(is_near == (near == 0), low, high)

    pick = spread(named) * (spread(earlier) == slot).astype(f32)
    weights_ref[...] = spread(gates) * pick
    packed = lax.dot_general(
        pick.astype(bf16), normed, (((0,), (0,)), ((), ())), preferred_element_type=f32
    )
    near_ref[0] = packed[:CAP].astype(bf16)
    far_ref[0] = packed[CAP:].astype(bf16)


def combine(values, weights_ref, returned):
    split = lax.axis_size("expert") // E_WIN
    blocks = [ref[index].astype(f32) for ref in returned for index in range(ref.shape[0])]
    result = values
    for side, group in enumerate((blocks[:split], blocks[split:])):
        total = group[0]
        for block in group[1:]:
            total = total + block
        for slot in range(CAP):
            column = side * CAP + slot
            result = result + weights_ref[:, column:column + 1] * total[slot:slot + 1, :]
    return result.astype(bf16)


def add_kernel(*refs):
    total = refs[0][...].astype(f32)
    for ref in refs[1:-1]:
        total = total + ref[...].astype(f32)
    refs[-1][...] = total.astype(bf16)


def first_kernel(tokens, ids_own, ids_other, gain_own, gain_other, router_own, router_other, *refs):
    outs, (stream, gain, router, sems) = refs[:3], refs[3:]
    copies = [
        pltpu.make_async_copy(tokens.at[lax.axis_index("section")], stream, sems.at[0]),
        pltpu.make_async_copy(gain_own, gain, sems.at[1]),
        pltpu.make_async_copy(router_own, router, sems.at[2]),
    ]
    for copy in copies:
        copy.start()
    for copy in copies:
        copy.wait()
    prepare(
        stream[...].astype(f32), 0, ids_own, ids_other, gain, gain_other, router, router_other, *outs
    )


def middle_kernel(count, layer, tokens, *refs):
    returned, refs = refs[:count], refs[count:]
    weights, refs = refs[0], refs[1:]
    params, outs = refs[:6], refs[6:]
    stream = combine(tokens[lax.axis_index("section")].astype(f32), weights, returned)
    outs[0][...] = stream
    prepare(stream.astype(f32), layer, *params, *outs[1:])


def final_kernel(count, stream, *refs):
    returned, weights, out = refs[:count], refs[count], refs[count + 1]
    out[0] = combine(stream[...].astype(f32), weights, returned)


def select_kernel(layer, own, crossed, *outs):
    mine = lax.axis_index("section") == layer
    row = 0
    pieces = [(out, index) for out in outs for index in range(out.shape[0])]
    for low in range(0, len(pieces), 2):
        lines = pl.ds(low * CAP, 2 * CAP)
        value = jnp.where(mine, own[lines, :].astype(f32), crossed[lines, :].astype(f32))
        for at, (out, index) in enumerate(pieces[low:low + 2]):
            out[index] = value[at * CAP:(at + 1) * CAP].astype(bf16)


def expert_kernel(layer, count, *refs):
    inputs, refs = refs[:2 * count], refs[2 * count:]
    gate_ref, up_hbm, down_hbm, own_out, other_out = refs[:5]
    rows_ref, up_buf, down_buf, gate_sum, up_sum, hidden_ref, total, up_sems, down_sems = refs[5:]
    half, width = own_out.shape
    real, padded = 2 * half, rows_ref.shape[0]
    units = gate_ref.shape[1]
    up_slots, depth, _ = up_buf.shape
    down_slots, block, _ = down_buf.shape
    steps, blocks = width // depth, units // block
    strip = width // 6

    def fetch_up(index, slot):
        lines = pl.ds(pl.multiple_of(index * depth, depth), depth)
        return pltpu.make_async_copy(up_hbm.at[lines], up_buf.at[slot], up_sems.at[slot])

    def fetch_down(index):
        slot = index % down_slots
        return pltpu.make_async_copy(
            down_hbm.at[pl.ds(index * block, block)], down_buf.at[slot], down_sems.at[slot]
        )

    for slot in range(up_slots):
        fetch_up(slot, slot).start()
    for index in range(min(down_slots, blocks)):
        fetch_down(index).start(priority=1)
    places = [(ref, index) for ref in inputs for index in range(ref.shape[0])]
    for low in range(0, len(places), 2):
        pair = [ref[index].astype(f32) for ref, index in places[low:low + 2]]
        lines = jnp.concatenate(pair, axis=0).astype(bf16)
        for start in range(0, padded, real):
            rows_ref[pl.ds(start + low * CAP, 2 * CAP), :] = lines

    def gate_part(index, fresh=False):
        lines = pl.ds(pl.multiple_of(index * depth, depth), depth)
        value = jnp.dot(rows_ref[:, lines], gate_ref[lines, :], preferred_element_type=f32)[:real]
        gate_sum[...] = value if fresh else gate_sum[...] + value

    def up_part(index, slot):
        lines = pl.ds(pl.multiple_of(index * depth, depth), depth)
        value = jnp.dot(rows_ref[:, lines], up_buf[slot], preferred_element_type=f32)[:real]
        up_sum[...] += value

    up_sum[...] = jnp.zeros_like(up_sum)
    gate_part(0, True)
    turns = steps // up_slots

    def turn_of(turn, last):
        for slot in range(up_slots):
            index = turn * up_slots + slot
            fetch_up(index, slot).wait()
            up_part(index, slot)
            if not (last and slot == up_slots - 1):
                gate_part(index + 1)
            if not last:
                fetch_up(index + up_slots, slot).start()

    @pl.loop(0, turns - 1)
    def _(turn):
        turn_of(turn, False)

    turn_of(turns - 1, True)
    for start in range(0, padded, real):
        hidden_ref[start:start + real, :] = (
            jax.nn.silu(gate_sum[...]) * up_sum[...]
        ).astype(bf16)

    for index in range(blocks):
        fetch_down(index).wait()
        hidden = hidden_ref[:, pl.ds(index * block, block)]
        for start in range(0, width, strip):
            columns = pl.ds(start, strip)
            value = jnp.dot(
                hidden, down_buf[index % down_slots, :, columns], preferred_element_type=f32
            )[:real]
            if index > 0:
                value += total[:, columns]
            if index == blocks - 1:
                value = value.astype(bf16)
                own_out[:, columns] = value[:half]
                other_out[:, columns] = value[half:]
            else:
                total[:, columns] = value
        if index + down_slots < blocks:
            fetch_down(index + down_slots).start(priority=1)


def call(kernel, outs, args, specs=None, limit=2 * MIB, scratch=(), flops=10**6):
    many = isinstance(outs, (tuple, list))
    return pl.pallas_call(
        kernel,
        out_shape=tuple(outs) if many else outs,
        in_specs=specs or [VMEM] * len(args),
        out_specs=(VMEM,) * len(outs) if many else VMEM,
        scratch_shapes=list(scratch),
        compiler_params=pltpu.CompilerParams(vmem_limit_bytes=limit),
        cost_estimate=pl.CostEstimate(flops=flops, bytes_accessed=10**5, transcendentals=0),
    )(*args)


def shape(*sizes, dtype=bf16):
    return jax.ShapeDtypeStruct(sizes, dtype)


def experts(layer, own, other, gate_matrix, up_matrix, down_matrix):
    half = CAP * sum(block.shape[0] for block in own)
    width, units = gate_matrix.shape
    block = min(256, units)
    depth = width // 12
    up_slots, down_slots = 4, min(5, units // block)
    padded = max(2 * half, 128)
    scratch = (
        pltpu.VMEM((padded, width), bf16),
        pltpu.VMEM((up_slots, depth, units), bf16),
        pltpu.VMEM((down_slots, block, width), bf16),
        pltpu.VMEM((2 * half, units), f32),
        pltpu.VMEM((2 * half, units), f32),
        pltpu.VMEM((padded, units), bf16),
        pltpu.VMEM((2 * half, width), f32),
        pltpu.SemaphoreType.DMA((up_slots,)),
        pltpu.SemaphoreType.DMA((down_slots,)),
    )
    count = len(own)
    limit = 2 * up_slots * depth * units + 2 * down_slots * block * width
    limit += 20 * half * width + 24 * half * units - (0 if half > 64 else 1 * MIB)
    args = (
        *own,
        *other,
        gate_matrix,
        pltpu.with_memory_space_constraint(up_matrix, pltpu.HBM),
        pltpu.with_memory_space_constraint(down_matrix, pltpu.HBM),
    )
    return call(
        lambda *refs: expert_kernel(layer, count, *refs),
        (shape(half, width), shape(half, width)),
        args,
        [VMEM] * (2 * count + 1) + [ANY] * 2,
        limit,
        scratch,
        12 * half * width * units,
    )


def across(value, step):
    devices = lax.axis_size("expert")
    return lax.ppermute(value, "expert", [(i, i ^ step) for i in range(devices)])


def exchange(near, far):
    devices = lax.axis_size("expert")
    split = devices // E_WIN
    if devices <= DIRECT:
        cross = across(far, split)
        return [
            block if step == 0 else across(block, step)
            for block in (near, cross)
            for step in range(split)
        ]
    low = lax.axis_index("expert") < split
    first, second = jnp.where(low, near, far), jnp.where(low, far, near)
    outgoing = jnp.concatenate([jnp.repeat(first, split, axis=0), jnp.repeat(second, split, axis=0)])
    return [lax.all_to_all(outgoing, "expert", 0, 0, tiled=True)]


def give_back(blocks):
    devices = lax.axis_size("expert")
    split = devices // E_WIN
    if devices <= DIRECT:
        far = [blocks[split]] + [across(blocks[split + step], step) for step in range(1, split)]
        near = [blocks[0]] + [across(blocks[step], step) for step in range(1, split)]
        total = call(add_kernel, shape(*far[0].shape), far)
        return near + [across(total, split)]
    returned = lax.all_to_all(blocks[0], "expert", 0, 0, tiled=True)
    turned = jnp.roll(returned, split, axis=0)
    return [jnp.where(lax.axis_index("expert") < split, returned, turned)]


def body(tokens, expert_ids, norm_gain, router, w_gate, w_up, w_down):
    layers = lax.axis_size("section")
    width = tokens.shape[-1]
    rows = tokens.shape[1]
    ids_own, gain_own, router_own = expert_ids[0], norm_gain, router[0].T
    params = (ids_own, swap(ids_own), gain_own, swap(gain_own), router_own, swap(router_own))
    slots = (shape(1, CAP, width), shape(1, CAP, width), shape(rows, E_WIN * CAP, dtype=f32))
    hbm = [pltpu.with_memory_space_constraint(x, pltpu.HBM) for x in (tokens, gain_own, router_own)]
    near, far, weights = call(
        first_kernel,
        slots,
        (hbm[0], *params[:2], hbm[1], params[3], hbm[2], params[5]),
        [ANY, VMEM, VMEM, ANY, VMEM, ANY, VMEM],
        scratch=[
            pltpu.VMEM((rows, width), bf16),
            pltpu.VMEM(gain_own.shape, bf16),
            pltpu.VMEM(router_own.shape, bf16),
            pltpu.SemaphoreType.DMA((3,)),
        ],
        flops=10**12,
    )
    stream = tokens
    for layer in range(layers):
        own = exchange(near, far)
        other = [swap(block) for block in own]
        own_terms, other_terms = experts(layer, own, other, w_gate[0], w_up[0], w_down[0])
        crossed = swap(other_terms)
        count = len(own)
        extra = 24 * CAP * sum(block.shape[0] for block in own) * width
        chosen = call(
            lambda *refs, layer=layer: select_kernel(layer, *refs),
            [shape(*block.shape) for block in own],
            (own_terms, crossed),
            limit=2 * MIB + extra // 2,
        )
        returned = give_back(chosen)
        count = len(returned)
        if layer < layers - 1:
            stream, near, far, weights = call(
                lambda *refs, layer=layer: middle_kernel(count, layer + 1, *refs),
                (shape(rows, width), *slots),
                (stream, *returned, weights, *params),
                limit=2 * MIB + extra // 2,
                flops=10**12,
            )
        else:
            return call(
                lambda *refs: final_kernel(count, *refs),
                shape(1, rows, width),
                (stream, *returned, weights),
                limit=2 * MIB + extra // 2,
            )


def solution(mesh):
    in_specs = (
        P(None, ("groups", "expert"), None),
        P("section", None, ("groups", "expert"), None),
        P("section", None),
        P("section", None, None),
        P("section", None, "expert"),
        P("section", None, "expert"),
        P("section", "expert", None),
    )
    out_specs = P("section", ("groups", "expert"), None)
    return jax.shard_map(body, mesh=mesh, in_specs=in_specs, out_specs=out_specs, check_vma=False)
```
